16 devices in a mesh: dp: 2 (over z), vp: 8 (over y, x, core).
Axes of the slice: x: 2, y: 2, z: 2, core: 2. Of those that a mesh axis runs over, the one named last changes fastest.
Arguments:
- hidden: bfloat16 [4096, 4096], P(('dp', 'vp')), parts along dimension 0
- labels: int32 [4096], P(('dp', 'vp')), parts along dimension 0
- loss_weight: float32 [4096], P(('dp', 'vp')), parts along dimension 0
- norm_gain: float32 [4096], replicated
- w_unembed: bfloat16 [4096, 32128], P(None, 'vp')
Outputs:
- output 1: float32 [2], P('dp'), parts along dimension 0
- output 2: bfloat16 [4096, 4096], P(('dp', 'vp')), parts along dimension 0
- output 3: float32 [8192, 32128], P('dp', 'vp'), parts along dimension 0
- output 4: float32 [8192], P('dp'), parts along dimension 0
There are 2 independent parts. The reference program is written for one: setup_inputs(seed, part) draws one part's arguments, and reference() takes and returns one part's arrays. A program takes and returns all parts, laid end to end along the dimension named above; an argument that names none is the same for every part.
All inputs are finite; a program needn't handle non-finite values.
Results may differ from the reference program's by a relative error of at most 0.001.
Values are sent between devices in bfloat16 or wider.
A program may use at most 1 GiB of HBM per device.

```python
import jax
import jax.numpy as jnp
from jax import lax

D = 4096
V = 32000
PAD_COLS = 128
TOK_DEV = 256
GROUP_SIZE = 8
VOCAB_PAD = V + PAD_COLS
TOKENS = TOK_DEV * GROUP_SIZE
LOW_IDS = V // 64
NORM_EPS = 1e-5


def setup_inputs(seed: int = 0, part: int = 0) -> dict:
    base_key = jax.random.key(seed)
    shared_key, parts_key = jax.random.split(base_key)
    part_key = jax.random.fold_in(parts_key, part)
    key_hid, key_pick, key_low, key_any, key_pad, key_wt = jax.random.split(part_key, 6)
    key_gain, key_unemb = jax.random.split(shared_key)
    hidden = jax.random.normal(key_hid, (TOKENS, D), jnp.float32).astype(jnp.bfloat16)
    tok_ids = jnp.arange(TOKENS)
    pick_low = jax.random.randint(key_pick, (TOKENS,), 0, 2)
    low_ids = jax.random.randint(key_low, (TOKENS,), 0, LOW_IDS)
    any_ids = jax.random.randint(key_any, (TOKENS,), 0, V)
    labels = jnp.where(pick_low == 0, low_ids, any_ids)
    labels = jnp.where(tok_ids == TOKENS - 1, V - 1, labels).astype(jnp.int32)
    pad_draw = jax.random.randint(key_pad, (TOKENS,), 0, 8)
    is_pad = (pad_draw == 0) & (tok_ids > 0)
    weight_val = jax.random.uniform(key_wt, (TOKENS,), jnp.float32, 0.25, 1.75)
    loss_weight = jnp.where(is_pad, 0.0, weight_val).astype(jnp.float32)
    norm_gain = 1.0 + 0.25 * jax.random.normal(key_gain, (D,), jnp.float32)
    w_unembed = (jax.random.normal(key_unemb, (D, VOCAB_PAD), jnp.float32) * (2.0 * D ** -0.5)).astype(jnp.bfloat16)
    return {"hidden": hidden, "labels": labels, "loss_weight": loss_weight, "norm_gain": norm_gain, "w_unembed": w_unembed}


def reference(hidden, labels, loss_weight, norm_gain, w_unembed):
    x_float = hidden.astype(jnp.float32)
    inv_rms = lax.rsqrt(jnp.mean(x_float * x_float, axis=-1, keepdims=True) + NORM_EPS)
    x_norm = x_float * inv_rms
    normed = (x_norm * norm_gain).astype(jnp.bfloat16)
    tok_scale = loss_weight / jnp.sum(loss_weight)
    col_ids = jnp.arange(VOCAB_PAD)[None, :]

    def block_step(d_unembed, block_in):
        normed_blk, label_blk, scale_blk = block_in
        logits = jnp.dot(normed_blk, w_unembed, preferred_element_type=jnp.float32)
        logits = jnp.where(col_ids < V, logits, -jnp.inf)
        is_target = col_ids == label_blk[:, None]
        row_max = jnp.max(logits, axis=1, keepdims=True)
        log_norm = row_max + jnp.log(jnp.sum(jnp.exp(logits - row_max), axis=1, keepdims=True))
        target = jnp.sum(jnp.where(is_target, logits, 0.0), axis=1, keepdims=True)
        tok_loss = (log_norm - target)[:, 0] * scale_blk
        d_logits = ((jnp.exp(logits - log_norm) - jnp.where(is_target, 1.0, 0.0)) * scale_blk[:, None]).astype(jnp.bfloat16)
        d_unembed = d_unembed + jnp.dot(normed_blk.T, d_logits, preferred_element_type=jnp.float32)
        d_normed = jnp.dot(d_logits, w_unembed.T, preferred_element_type=jnp.float32)
        return d_unembed, (tok_loss, d_normed)

    blocks = (normed.reshape(GROUP_SIZE, TOK_DEV, D), labels.reshape(GROUP_SIZE, TOK_DEV), tok_scale.reshape(GROUP_SIZE, TOK_DEV))
    d_unembed, (tok_loss, d_normed) = lax.scan(block_step, jnp.zeros((D, VOCAB_PAD), jnp.float32), blocks)
    d_normed = d_normed.reshape(TOKENS, D)
    mean_loss = jnp.sum(tok_loss).reshape(1)
    grad_hat = d_normed * norm_gain
    d_input = inv_rms * (grad_hat - x_norm * jnp.mean(grad_hat * x_norm, axis=-1, keepdims=True))
    d_norm_gain = jnp.sum(d_normed * x_norm, axis=0)
    return mean_loss, d_input.astype(jnp.bfloat16), d_unembed, d_norm_gain
```

```python
import jax
import jax.numpy as jnp
from jax import lax
from jax.sharding import PartitionSpec as P

NORM_EPS = 1e-5
PAD_COLS = 128


def solution(mesh):
    n = mesh.shape["vp"]

    def swap(v, mask):
        return lax.ppermute(v, "vp", [(i, i ^ mask) for i in range(n)])

    def local_step(hidden, labels, loss_weight, norm_gain, w_local):
        rows, dim = hidden.shape
        half = rows // 2
        dhalf = dim // 2
        vocab_local = w_local.shape[1]
        vocab_real = vocab_local * n - PAD_COLS
        me = lax.axis_index("vp")
        x_float = hidden.astype(jnp.float32)
        inv_rms = lax.rsqrt(jnp.mean(x_float * x_float, axis=-1, keepdims=True) + NORM_EPS)
        x_norm = x_float * inv_rms
        normed = (x_norm * norm_gain).astype(jnp.bfloat16)

        r0 = normed
        r2a, r4a = swap(r0[:half], 2), swap(r0[:half], 4)
        r2b, r4b = swap(r0[half:], 2), swap(r0[half:], 4)
        r1 = swap(r0, 1)
        r3a, r5a = swap(r2a, 1), swap(r4a, 1)
        r3b, r5b = swap(r2b, 1), swap(r4b, 1)
        r6a, r6b = swap(r2a, 4), swap(r4b, 2)
        r7a, r7b = swap(r6a, 1), swap(r6b, 1)
        a_parts = [
            jnp.concatenate([r0, r1]),
            jnp.concatenate([r2a, r3a, r4a, r5a]),
            jnp.concatenate([r2b, r3b, r4b, r5b]),
            jnp.concatenate([r6a, r6b, r7a, r7b]),
        ]

        side = jnp.stack([labels.astype(jnp.float32), loss_weight])[None]
        side = jnp.concatenate([side, swap(side, 1)])
        side = jnp.concatenate([side, swap(side, 2)])
        side = jnp.concatenate([side, swap(side, 4)])
        weight_sum = jnp.sum(side[:, 1])

        def group(v):
            return [
                jnp.concatenate([v[0], v[1]]),
                jnp.concatenate([v[2, :half], v[3, :half], v[4, :half], v[5, :half]]),
                jnp.concatenate([v[2, half:], v[3, half:], v[4, half:], v[5, half:]]),
                jnp.concatenate([v[6], v[7]]),
            ]

        labels_g = group(side[:, 0].astype(jnp.int32))
        scale_g = group(side[:, 1] / weight_sum)

        col_ids = me * vocab_local + lax.broadcasted_iota(jnp.int32, (1, vocab_local), 1)
        logits_g, stats_g = [], []
        for a_part, label in zip(a_parts, labels_g):
            logits = jnp.dot(a_part, w_local, preferred_element_type=jnp.float32)
            logits = jnp.where(col_ids < vocab_real, logits, -jnp.inf)
            row_max = jnp.max(logits, axis=1)
            sum_exp = jnp.sum(jnp.exp(logits - row_max[:, None]), axis=1)
            target = jnp.sum(jnp.where(col_ids == label[:, None], logits, 0.0), axis=1)
            logits_g.append(logits)
            stats_g.append((row_max, sum_exp, target))

        def combine(s, t):
            row_max = jnp.maximum(s[0], t[0])
            return jnp.stack([
                row_max,
                s[1] * jnp.exp(s[0] - row_max) + t[1] * jnp.exp(t[0] - row_max),
                s[2] + t[2],
            ])

        def ungroup(g):
            q = [v.reshape(4, half) for v in g]
            return jnp.stack([
                g[0][:rows], g[0][rows:],
                jnp.concatenate([q[1][0], q[2][0]]), jnp.concatenate([q[1][1], q[2][1]]),
                jnp.concatenate([q[1][2], q[2][2]]), jnp.concatenate([q[1][3], q[2][3]]),
                g[3][:rows], g[3][rows:],
            ])

        stats = jnp.stack([ungroup([s[k] for s in stats_g]) for k in range(3)])
        for mask in (1, 2, 4):
            other = swap(stats, mask)
            other = jnp.stack([other[:, r ^ mask] for r in range(n)], axis=1)
            stats = combine(stats, other)
        log_norm = stats[0] + jnp.log(stats[1])
        mean_loss = jnp.sum(side[:, 1] / weight_sum * (log_norm - stats[2])).reshape(1)

        dz_g = []
        for logits, label, scale, norm in zip(logits_g, labels_g, scale_g, group(log_norm)):
            prob = jnp.exp(logits - norm[:, None])
            hot = jnp.where(col_ids == label[:, None], 1.0, 0.0)
            dz_g.append(((prob - hot) * scale[:, None]).astype(jnp.bfloat16))

        def back(dz):
            return lax.dot_general(dz, w_local, (((1,), (1,)), ((), ())), preferred_element_type=jnp.float32)

        p67 = back(dz_g[3])
        q6 = p67[:rows] + swap(p67[rows:], 1)
        x6, y6 = swap(q6[:, :dhalf], 2), swap(q6[:, dhalf:], 4)
        pa = back(dz_g[1])
        pb = back(dz_g[2])
        q2a, q2b = pa[:half] + swap(pa[half:2 * half], 1), pb[:half] + swap(pb[half:2 * half], 1)
        q4a, q4b = pa[2 * half:3 * half] + swap(pa[3 * half:], 1), pb[2 * half:3 * half] + swap(pb[3 * half:], 1)
        q2, q4 = jnp.concatenate([q2a, q2b]), jnp.concatenate([q4a, q4b])
        x2, y4 = swap(q2[:, :dhalf], 2), swap(q4[:, dhalf:], 4)
        s4 = swap(q4[:, :dhalf] + x6, 4)
        t2 = swap(q2[:, dhalf:] + y6, 2)
        p01 = back(dz_g[0])
        q0 = p01[:rows] + swap(p01[rows:], 1)
        d_normed = jnp.concatenate([q0[:, :dhalf] + x2 + s4, q0[:, dhalf:] + y4 + t2], axis=1)

        d_unembed = lax.dot_general(
            jnp.concatenate(a_parts), jnp.concatenate(dz_g), (((0,), (0,)), ((), ())), preferred_element_type=jnp.float32)

        grad_hat = d_normed * norm_gain
        d_input = inv_rms * (grad_hat - x_norm * jnp.mean(grad_hat * x_norm, axis=-1, keepdims=True))
        d_norm_gain = jnp.sum(d_normed * x_norm, axis=0)
        for mask in (1, 2, 4):
            d_norm_gain = d_norm_gain + swap(d_norm_gain, mask)
        return mean_loss, d_input.astype(jnp.bfloat16), d_unembed, d_norm_gain

    return jax.shard_map(
        local_step,
        mesh=mesh,
        in_specs=(P(("dp", "vp"), None), P(("dp", "vp")), P(("dp", "vp")), P(None), P(None, "vp")),
        out_specs=(P("dp"), P(("dp", "vp"), None), P("dp", "vp"), P("dp")),
        check_vma=False,
    )
```

```python
import functools

import jax
import jax.numpy as jnp
from jax import lax
from jax.experimental import pallas as pl
from jax.experimental.pallas import tpu as pltpu
from jax.sharding import PartitionSpec as P


NORM_EPS = 1e-5
PAD_COLS = 128
BLK = 512
F32 = jnp.float32
BF16 = jnp.bfloat16


ANY = pl.BlockSpec(memory_space=pl.ANY)


def whole(shape):
    return pl.BlockSpec(shape, lambda *_: (0,) * len(shape))


def params(n_axes):
    return pltpu.CompilerParams(
        dimension_semantics=("arbitrary",) * n_axes, vmem_limit_bytes=60 * 1024 * 1024)


LOWEST = -3.4028234663852886e38


def fwd_body(k, n_parts, blk, limit_ref, wt_ref, *refs):
    a_refs = refs[:n_parts]
    z_ref, stat_ref, hold_ref = refs[-3:]
    step, steps = pl.program_id(0), pl.num_programs(0)
    pairs = [a_refs[i:i + 2] for i in range(0, n_parts, 2)]
    wide = 2 * a_refs[0].shape[0]

    def dots():
        for i, (lo, hi) in enumerate(pairs):
            a = jnp.concatenate([lo[...], hi[...]], axis=0)
            hold_ref[:, i * wide:(i + 1) * wide] = lax.dot_general(
                wt_ref[...], a, (((1,), (1,)), ((), ())), preferred_element_type=F32)

    def finish():
        for i in range(len(pairs)):
            cols = slice(i * wide, (i + 1) * wide)
            z = hold_ref[:, cols]
            col = (step - 1) * blk + lax.broadcasted_iota(jnp.int32, z.shape, 0)
            z = jnp.where(col < limit_ref[0], z, -jnp.inf)
            z_ref[:, cols] = z
            old = stat_ref[k:k + 1, cols]
            new = jnp.maximum(old, jnp.max(z, axis=0, keepdims=True))
            total = jnp.sum(jnp.exp(z - new), axis=0, keepdims=True)
            stat_ref[k:k + 1, cols] = new
            stat_ref[4 + k:5 + k, cols] = stat_ref[4 + k:5 + k, cols] * jnp.exp(old - new) + total

    @pl.when(step == 0)
    def _():
        stat_ref[...] = jnp.zeros(stat_ref.shape, F32) if k == 0 else refs[n_parts][...]
        stat_ref[k:k + 1, :] = jnp.full((1, stat_ref.shape[1]), LOWEST, F32)
        stat_ref[4 + k:5 + k, :] = jnp.zeros((1, stat_ref.shape[1]), F32)
        dots()

    @pl.when((step > 0) & (step < steps - 1))
    def _():
        finish()
        dots()

    pl.when(step == steps - 1)(finish)


def fwd_call(k, parts, wt, limit, stats):
    vocab, dim = wt.shape
    toks = sum(p.shape[0] for p in parts)
    blocks = pl.cdiv(vocab, BLK)
    return pl.pallas_call(
        functools.partial(fwd_body, k, len(parts), BLK),
        grid=(blocks + 1,),
        in_specs=[pl.BlockSpec(memory_space=pltpu.SMEM), pl.BlockSpec((BLK, dim), lambda j: (jnp.minimum(j, blocks - 1), 0))]
        + [whole(p.shape) for p in parts] + [whole((8, toks))] * len(stats),
        out_specs=[pl.BlockSpec((BLK, toks), lambda j: (jnp.maximum(j - 1, 0), 0)), whole((8, toks))],
        out_shape=[jax.ShapeDtypeStruct((vocab, toks), F32), jax.ShapeDtypeStruct((8, toks), F32)],
        scratch_shapes=[pltpu.VMEM((BLK, toks), F32)],
        compiler_params=params(1),
        cost_estimate=pl.CostEstimate(
            flops=2 * vocab * dim * toks, bytes_accessed=vocab * dim * 2 + vocab * toks * 4,
            transcendentals=vocab * toks),
        name="fwd",
    )(limit, wt, *parts, *stats)


TILE = 1024


def mix(first, keep_ref, got_ref, outs):
    q = keep_ref[...] + got_ref[...]
    dhalf = q.shape[1] // 2

    @pl.when(first)
    def _():
        outs[0][...], outs[1][...] = q[:, :dhalf], q[:, dhalf:]

    @pl.when(jnp.logical_not(first))
    def _():
        outs[2][...], outs[3][...] = q[:, :dhalf], q[:, dhalf:]


def back_body(k, mixing, blk, vocab, label_ref, lse_ref, scale_ref, loss_ref, z_ref, wt_ref, *refs):
    dz_ref, keep_ref, send_ref, lost_ref = refs[-10:-6] if mixing else refs[-6:-2]
    acc_ref, sem = refs[-2:]
    step, steps = pl.program_id(0), pl.num_programs(0)
    tail = vocab - (vocab // blk) * blk or blk
    rows, dim = keep_ref.shape
    row = slice(k, k + 1)

    @pl.when(step == 0)
    def _():
        acc_ref[...] = jnp.zeros_like(acc_ref)
        lost_ref[...] = loss_ref[...]

    if mixing:
        mix(step < steps // 2, refs[0], refs[1], refs[-6:-2])

    def run(size, leave):
        z = z_ref[:size]
        col = step * blk + lax.broadcasted_iota(jnp.int32, z.shape, 0)
        hit = col == label_ref[row]
        scale = scale_ref[row]
        dz = ((jnp.exp(z - lse_ref[row]) - jnp.where(hit, 1.0, 0.0)) * scale).astype(BF16)
        dz_ref[:size] = dz
        lost = jnp.sum(jnp.where(hit, z, 0.0), axis=0, keepdims=True) * scale
        wide = lost_ref.shape[1]
        lost_ref[0:1] = lost_ref[0:1] - sum(lost[:, i:i + wide] for i in range(0, lost.shape[1], wide))
        copies = []
        for t in range(dim // TILE):
            cols = slice(t * TILE, (t + 1) * TILE)
            acc_ref[:, cols] += lax.dot_general(
                dz, wt_ref[:size, cols], (((0,), (0,)), ((), ())), preferred_element_type=F32)
            if leave:
                for h, out in enumerate((keep_ref, send_ref)):
                    copies.append(pltpu.make_async_copy(
                        acc_ref.at[h * rows:(h + 1) * rows, cols], out.at[:, cols], sem.at[2 * t + h]))
                    copies[-1].start()
        for c in copies:
            c.wait()

    pl.when(step < steps - 1)(lambda: run(blk, False))
    pl.when(step == steps - 1)(lambda: run(tail, True))


def back_call(k, z, wt, label, lse, scale, loss, shared, pair):
    vocab, dim = wt.shape
    toks = z.shape[1]
    rows = toks // 2
    steps = pl.cdiv(vocab, BLK)
    mixing = bool(pair)
    in_specs = [whole((8, toks))] * 3 + [whole((8, 128)), pl.BlockSpec((BLK, toks), lambda j: (j, 0)),
                                         pl.BlockSpec((BLK, dim), lambda j: (j, 0))]
    out_specs = [pl.BlockSpec((BLK, toks), lambda j: (j, k)), ANY, ANY, whole((8, 128))]
    out_shape = [jax.ShapeDtypeStruct((vocab, 4 * toks), BF16), jax.ShapeDtypeStruct((rows, dim), F32),
                 jax.ShapeDtypeStruct((rows, dim), F32), jax.ShapeDtypeStruct((8, 128), F32)]
    if mixing:
        blk, mid, dhalf = rows // steps, steps // 2, dim // 2
        low = pl.BlockSpec((blk, dhalf), lambda j: (jnp.minimum(j, mid - 1), 0))
        high = pl.BlockSpec((blk, dhalf), lambda j: (jnp.maximum(j - mid, 0), 0))
        in_specs += [pl.BlockSpec((blk, dim), lambda j: (j, 0))] * 2
        out_specs += [low, low, high, high]
        out_shape += [jax.ShapeDtypeStruct((rows // 2, dhalf), F32)] * 4
    args = [label, lse, scale, loss, z, wt, *pair, *shared]
    return pl.pallas_call(
        functools.partial(back_body, k, mixing, BLK, vocab),
        grid=(steps,),
        in_specs=in_specs + [ANY] * len(shared),
        out_specs=out_specs,
        out_shape=out_shape,
        input_output_aliases={len(args) - 1: 0} if shared else {},
        scratch_shapes=[pltpu.VMEM((toks, dim), F32), pltpu.SemaphoreType.DMA((2 * dim // TILE,))],
        compiler_params=params(1),
        cost_estimate=pl.CostEstimate(
            flops=2 * vocab * dim * toks, bytes_accessed=vocab * dim * 2 + vocab * toks * 6,
            transcendentals=vocab * toks),
        name="back",
    )(*args)


def weight_body(n_parts, dz_ref, *refs):
    a_refs, out_ref, tick_ref = refs[:n_parts], refs[-2], refs[-1]
    tick_ref[...] = jnp.zeros_like(tick_ref)

    @pl.loop(0, out_ref.shape[1] // TILE)
    def _(k):
        cols = pl.ds(pl.multiple_of(k * TILE, TILE), TILE)
        a = jnp.concatenate([r[:, cols] for r in a_refs], axis=0)
        out_ref[:, cols] = jnp.dot(dz_ref[...], a, preferred_element_type=F32)


def weight_call(dz, parts):
    vocab, toks = dz.shape
    dim = parts[0].shape[1]
    rows, cols = 1024, dim // 2
    return pl.pallas_call(
        functools.partial(weight_body, len(parts)),
        grid=(dim // cols, pl.cdiv(vocab, rows)),
        in_specs=[pl.BlockSpec((rows, toks), lambda n, j: (j, 0))]
        + [pl.BlockSpec((p.shape[0], cols), lambda n, j: (0, n)) for p in parts],
        out_specs=[pl.BlockSpec((rows, cols), lambda n, j: (j, n)), whole((8, 128))],
        out_shape=[jax.ShapeDtypeStruct((vocab, dim), F32), jax.ShapeDtypeStruct((8, 128), F32)],
        compiler_params=params(2),
        cost_estimate=pl.CostEstimate(
            flops=2 * vocab * dim * toks, bytes_accessed=vocab * dim * 4 + vocab * toks * 4, transcendentals=0),
        name="dweight",
    )(dz, *parts)


def norm_body(hid_ref, gain_ref, lo_ref, hi_ref):
    step = pl.program_id(0)
    x = hid_ref[...].astype(F32)
    inv = lax.rsqrt(jnp.mean(x * x, axis=-1, keepdims=True) + NORM_EPS)
    a = (x * inv * gain_ref[...]).astype(BF16)

    @pl.when(step < pl.num_programs(0) // 2)
    def _():
        lo_ref[...] = a

    @pl.when(step >= pl.num_programs(0) // 2)
    def _():
        hi_ref[...] = a


def norm_call(hidden, gain, order):
    rows, dim = hidden.shape
    steps = 2
    blk, mid = rows // steps, steps // 2
    body = lambda *refs: norm_body(refs[0], refs[1], refs[-2], refs[-1])
    return pl.pallas_call(
        body,
        grid=(steps,),
        in_specs=[pl.BlockSpec((blk, dim), lambda i: (i, 0)), whole((1, dim))] + [ANY] * len(order),
        out_specs=[pl.BlockSpec((blk, dim), lambda i: (jnp.minimum(i, mid - 1), 0)),
                   pl.BlockSpec((blk, dim), lambda i: (jnp.maximum(i - mid, 0), 0))],
        out_shape=[jax.ShapeDtypeStruct((rows // 2, dim), BF16)] * 2,
        compiler_params=params(1),
        cost_estimate=pl.CostEstimate(flops=5 * rows * dim, bytes_accessed=rows * dim * 4, transcendentals=rows),
        name="norm",
    )(hidden, gain[None], *order)


def peer(me, mask):
    out = me
    for bit in (1, 2, 4):
        if mask & bit:
            out = out + bit * (1 - 2 * ((me // bit) % 2))
    return out


def push_all(n, sends, send_sem, recv_sem):
    me = lax.axis_index("vp")
    barrier = pltpu.get_barrier_semaphore()
    for m in range(1, n):
        pl.semaphore_signal(barrier, inc=1, device_id={"vp": peer(me, m)}, device_id_type=pl.DeviceIdType.MESH)
    pl.semaphore_wait(barrier, n - 1)
    copies = [
        pltpu.make_async_remote_copy(
            src_ref=src, dst_ref=got.at[m], send_sem=send_sem.at[i, m], recv_sem=recv_sem.at[i, m],
            device_id={"vp": peer(me, m)}, device_id_type=pl.DeviceIdType.MESH)
        for m in range(1, n) for i, (src, got) in enumerate(sends)
    ]
    for c in copies:
        c.start()
    for c in copies:
        c.wait()


def tree(v):
    while len(v) > 1:
        v = [v[i] + v[i + 1] for i in range(0, len(v), 2)]
    return v[0]


def sum_body(n, gain_ref, loss_ref, gain_out, loss_out, got_gain, got_loss, send_sem, recv_sem):
    push_all(n, [(gain_ref, got_gain), (loss_ref, got_loss)], send_sem, recv_sem)
    gain_out[...] = tree([gain_ref[...]] + [got_gain[m] for m in range(1, n)])
    loss_out[...] = tree([loss_ref[...]] + [got_loss[m] for m in range(1, n)])


LAYOUT = (
    ((0, 0), (0, 1), (1, 0), (1, 1)),
    ((2, 0), (4, 0), (3, 0), (5, 0)),
    ((2, 1), (4, 1), (3, 1), (5, 1)),
    ((6, 0), (6, 1), (7, 0), (7, 1)),
)


def stats_body(n, vocab, stat_ref, label_ref, weight_ref, label_out, lse_out, scale_out, loss_out,
               got_stat, got_label, got_weight, send_sem, recv_sem):
    push_all(n, [(stat_ref, got_stat), (label_ref, got_label), (weight_ref, got_weight)], send_sem, recv_sem)
    width = stat_ref.shape[1] // 4
    base = lax.axis_index("vp") * vocab
    place = {key: (k, i) for k, row in enumerate(LAYOUT) for i, key in enumerate(row)}
    pick = lambda own, got, m, *at: own[at] if m == 0 else got[(m,) + at]
    lanes = lambda i: slice(i * width, (i + 1) * width)
    one = lambda k: slice(k, k + 1)
    total_weight = tree([
        jnp.sum(pick(weight_ref, got_weight, m, slice(0, 2)), axis=(0, 1), keepdims=True) for m in range(n)])
    loss = jnp.zeros((1, width), F32)
    label_out[4:] = jnp.zeros((4, 4 * width), jnp.int32)
    lse_out[4:] = jnp.zeros((4, 4 * width), F32)
    scale_out[4:] = jnp.zeros((4, 4 * width), F32)
    for k, row in enumerate(LAYOUT):
        for i, (r, h) in enumerate(row):
            tops, sums = [], []
            for m in range(n):
                kk, ii = place[(r ^ m, h)]
                tops.append(pick(stat_ref, got_stat, m, one(kk), lanes(ii)))
                sums.append(pick(stat_ref, got_stat, m, one(4 + kk), lanes(ii)))
            top = functools.reduce(jnp.maximum, tops)
            lse = top + jnp.log(tree([s * jnp.exp(t - top) for s, t in zip(sums, tops)]))
            scale = pick(weight_ref, got_weight, r, one(h)) / total_weight
            lse_out[one(k), lanes(i)] = lse
            scale_out[one(k), lanes(i)] = scale
            label_out[one(k), lanes(i)] = pick(label_ref, got_label, r, one(h)) - base
            if r == 0:
                loss = loss + scale * lse
    loss_out[...] = jnp.zeros(loss_out.shape, F32)
    loss_out[0:1] = loss


def small_call(body, n, args, outs, ident):
    vm = pl.BlockSpec(memory_space=pltpu.VMEM)
    sems = [pltpu.SemaphoreType.DMA((len(args), n))] * 2
    return pl.pallas_call(
        body,
        in_specs=[vm] * len(args),
        out_specs=[vm] * len(outs),
        out_shape=outs,
        scratch_shapes=[pltpu.VMEM((n,) + v.shape, v.dtype) for v in args] + sems,
        compiler_params=pltpu.CompilerParams(collective_id=ident, has_side_effects=True),
        cost_estimate=pl.CostEstimate(flops=4000, bytes_accessed=4_000_000, transcendentals=0),
    )(*args)


def mix_body(keep_ref, got_ref, a_ref, b_ref):
    q = keep_ref[...] + got_ref[...]
    dhalf = q.shape[1] // 2
    a_ref[...], b_ref[...] = q[:, :dhalf], q[:, dhalf:]


def mix_call(keep, got):
    rows, dim = keep.shape
    steps = 4
    blk, dhalf = rows // steps, dim // 2
    full = pl.BlockSpec((blk, dim), lambda i: (i, 0))
    return pl.pallas_call(
        mix_body,
        grid=(steps,),
        in_specs=[full, full],
        out_specs=[pl.BlockSpec((blk, dhalf), lambda i: (i, 0))] * 2,
        out_shape=[jax.ShapeDtypeStruct((rows, dhalf), F32)] * 2,
        compiler_params=params(1),
        cost_estimate=pl.CostEstimate(flops=rows * dim, bytes_accessed=rows * dim * 12, transcendentals=0),
        name="mix",
    )(keep, got)


def second_body(keep2_ref, keep4_ref, got2_ref, got4_ref, sa_ref, ta_ref, xa_ref, xb_ref, ya_ref, yb_ref,
                x2_ref, y4_ref, s_ref, t_ref):
    dhalf = sa_ref.shape[1]
    q2 = keep2_ref[...] + got2_ref[...]
    q4 = keep4_ref[...] + got4_ref[...]
    x2_ref[...] = q2[:, :dhalf]
    y4_ref[...] = q4[:, dhalf:]
    s_ref[0] = sa_ref[...] + xa_ref[...]
    s_ref[1] = q4[:, :dhalf] + xb_ref[...]
    t_ref[0] = ta_ref[...] + ya_ref[...]
    t_ref[1] = q2[:, dhalf:] + yb_ref[...]


def second_call(keep, got, sa, ta, x, y):
    half, dhalf = sa.shape
    steps = 4
    blk = half // steps
    at = lambda width, off: pl.BlockSpec((blk, width), lambda i: (i + off, 0))
    two = pl.BlockSpec((2, blk, dhalf), lambda i: (0, i, 0))
    return pl.pallas_call(
        second_body,
        grid=(steps,),
        in_specs=[at(2 * dhalf, 0), at(2 * dhalf, steps), at(2 * dhalf, 0), at(2 * dhalf, steps), at(dhalf, 0), at(dhalf, 0),
                  at(dhalf, 0), at(dhalf, steps), at(dhalf, 0), at(dhalf, steps)],
        out_specs=[at(dhalf, 0), at(dhalf, 0), two, two],
        out_shape=[jax.ShapeDtypeStruct((half, dhalf), F32)] * 2 + [jax.ShapeDtypeStruct((2, half, dhalf), F32)] * 2,
        compiler_params=params(1),
        cost_estimate=pl.CostEstimate(flops=8 * half * dhalf, bytes_accessed=half * dhalf * 80, transcendentals=0),
        name="second",
    )(keep, keep, got, got, sa, ta, x, x, y, y)


def last_body(hid_ref, gain_ref, keep_ref, got_ref, x2a_ref, x2b_ref, s4_ref, y4a_ref, y4b_ref, t2_ref, tick_ref,
              dh_ref, dgain_ref):
    del tick_ref
    step = pl.program_id(0)
    dhalf = s4_ref.shape[1]

    def run(x2_ref, y4_ref):
        q = keep_ref[...] + got_ref[...]
        g = jnp.concatenate(
            [q[:, :dhalf] + x2_ref[...] + s4_ref[...], q[:, dhalf:] + y4_ref[...] + t2_ref[...]], axis=1)
        x = hid_ref[...].astype(F32)
        inv = lax.rsqrt(jnp.mean(x * x, axis=-1, keepdims=True) + NORM_EPS)
        norm = x * inv
        u = g * gain_ref[...]
        dh_ref[...] = (inv * (u - norm * jnp.mean(u * norm, axis=-1, keepdims=True))).astype(BF16)
        part = jnp.sum(g * norm, axis=0, keepdims=True)
        wide = dgain_ref.shape[1]
        for k in range(dgain_ref.shape[0]):
            piece = part[:, k * wide:(k + 1) * wide]
            dgain_ref[k:k + 1] = jnp.where(step == 0, piece, dgain_ref[k:k + 1] + piece)

    pl.when(step < pl.num_programs(0) // 2)(lambda: run(x2a_ref, y4a_ref))
    pl.when(step >= pl.num_programs(0) // 2)(lambda: run(x2b_ref, y4b_ref))


def last_call(hidden, gain, keep, got, x2a, x2b, s4, y4a, y4b, t2, tick):
    rows, dim = hidden.shape
    steps = 8
    blk, mid, dhalf = rows // steps, steps // 2, dim // 2
    row = lambda width: pl.BlockSpec((blk, width), lambda i: (i, 0))
    low = pl.BlockSpec((blk, dhalf), lambda i: (jnp.minimum(i, mid - 1), 0))
    high = pl.BlockSpec((blk, dhalf), lambda i: (jnp.maximum(i - mid, 0), 0))
    return pl.pallas_call(
        last_body,
        grid=(steps,),
        in_specs=[row(dim), whole((1, dim)), row(dim), row(dim), low, high, row(dhalf), low, high, row(dhalf), ANY],
        out_specs=[row(dim), whole((8, dim // 8))],
        out_shape=[jax.ShapeDtypeStruct((rows, dim), BF16), jax.ShapeDtypeStruct((8, dim // 8), F32)],
        compiler_params=params(1),
        cost_estimate=pl.CostEstimate(flops=20 * rows * dim, bytes_accessed=rows * dim * 20, transcendentals=rows),
        name="last",
    )(hidden, gain[None], keep, got, x2a, x2b, s4, y4a, y4b, t2, tick)


def solution(mesh):
    n = mesh.shape["vp"]

    def swap(v, mask):
        return lax.ppermute(v, "vp", [(i, i ^ mask) for i in range(n)])

    def compute(hidden, labels, loss_weight, norm_gain, w_local):
        rows, dim = hidden.shape
        half, dhalf = rows // 2, dim // 2
        wt = w_local.T
        vocab_local = wt.shape[0]
        vocab_real = vocab_local * n - PAD_COLS
        me = lax.axis_index("vp")

        limit = jnp.minimum(vocab_real - me * vocab_local, vocab_local).astype(jnp.int32).reshape(1)

        r0a, r0b = norm_call(hidden, norm_gain, [])
        r2a, r4a = swap(r0a, 2), swap(r0a, 4)
        r1a, r1b = swap(r0a, 1), swap(r0b, 1)
        r2b, r4b = swap(r0b, 2), swap(r0b, 4)
        r3a, r5a = swap(r2a, 1), swap(r4a, 1)
        r3b, r5b = swap(r2b, 1), swap(r4b, 1)
        r6a, r6b = swap(r2a, 4), swap(r4b, 2)
        r7a, r7b = swap(r6a, 1), swap(r6b, 1)
        groups = [[r0a, r0b, r1a, r1b], [r2a, r4a, r3a, r5a], [r2b, r4b, r3b, r5b], [r6a, r6b, r7a, r7b]]

        logits_g, stats = [], []
        for k, parts in enumerate(groups):
            logits, stat = fwd_call(k, parts, wt, limit, stats)
            logits_g.append(logits)
            stats = [stat]

        spec = jax.ShapeDtypeStruct
        label, lse, scale, loss = small_call(
            functools.partial(stats_body, n, vocab_local), n,
            [stats[0], labels.reshape(2, half), loss_weight.reshape(2, half)],
            [spec((8, 2 * rows), jnp.int32), spec((8, 2 * rows), F32), spec((8, 2 * rows), F32), spec((8, half), F32)],
            0)

        def back(k, loss, shared, pair):
            return back_call(k, logits_g[k], wt, label, lse, scale, loss, shared, pair)

        dz, keep3, send3, loss = back(3, loss, [], [])
        got3 = swap(send3, 1)
        dz, keep1, send1, loss = back(1, loss, [dz], [])
        q6x, q6y = mix_call(keep3, got3)
        x6, y6 = swap(q6x, 2), swap(q6y, 4)
        got1 = swap(send1, 1)
        dz, keep2, send2, loss = back(2, loss, [dz], [])
        got2 = swap(send2, 1)
        dz, keep0, send0, loss, x2a, ta, sa, y4a = back(0, loss, [dz], [keep1, got1])
        x2a, y4a = swap(x2a, 2), swap(y4a, 4)
        got0 = swap(send0, 1)
        x2b, y4b, s4, t2 = second_call(keep2, got2, sa, ta, x6, y6)
        x2b, y4b = swap(x2b, 2), swap(y4b, 4)
        s4, t2 = swap(s4, 4).reshape(rows, dhalf), swap(t2, 2).reshape(rows, dhalf)

        dwt, tick = weight_call(dz, [p for g in groups for p in g])
        d_input, d_gain = last_call(hidden, norm_gain, keep0, got0, x2a, x2b, s4, y4a, y4b, t2, tick)
        d_gain, loss = small_call(
            functools.partial(sum_body, n), n, [d_gain, loss], [spec(d_gain.shape, F32), spec(loss.shape, F32)], 1)
        return jnp.sum(loss[0]).reshape(1), d_input, dwt.T, d_gain.reshape(dim)

    return jax.shard_map(
        compute,
        mesh=mesh,
        in_specs=(P(("dp", "vp"), None), P(("dp", "vp")), P(("dp", "vp")), P(None), P(None, "vp")),
        out_specs=(P("dp"), P(("dp", "vp"), None), P("dp", "vp"), P("dp")),
        check_vma=False,
    )
```

```python
import functools

import jax
import jax.numpy as jnp
from jax import lax
from jax.experimental import pallas as pl
from jax.experimental.pallas import tpu as pltpu
from jax.sharding import PartitionSpec as P


NORM_EPS = 1e-5
PAD_COLS = 128
BLK = 512
VMEM = 67_043_328
F32 = jnp.float32
BF16 = jnp.bfloat16


ANY = pl.BlockSpec(memory_space=pl.ANY)


def whole(shape):
    return pl.BlockSpec(shape, lambda *_: (0,) * len(shape))


def params(n_axes):
    return pltpu.CompilerParams(
        dimension_semantics=("arbitrary",) * n_axes, vmem_limit_bytes=VMEM)


LOWEST = -3.4028234663852886e38


def fwd_body(k, n_parts, blk, limit_ref, wt_ref, *refs):
    a_refs = refs[:n_parts]
    z_ref, stat_ref = refs[-2:]
    step, steps = pl.program_id(0), pl.num_programs(0)
    pairs = [a_refs[i:i + 2] for i in range(0, n_parts, 2)]
    wide = 2 * a_refs[0].shape[0]

    @pl.when(step == 0)
    def _():
        stat_ref[...] = jnp.zeros(stat_ref.shape, F32) if k == 0 else refs[n_parts][...]
        stat_ref[k:k + 1, :] = jnp.full((1, stat_ref.shape[1]), LOWEST, F32)
        stat_ref[4 + k:5 + k, :] = jnp.zeros((1, stat_ref.shape[1]), F32)

    for i, (lo, hi) in enumerate(pairs):
        a = jnp.concatenate([lo[...], hi[...]], axis=0)
        z_ref[:, i * wide:(i + 1) * wide] = lax.dot_general(
            wt_ref[...], a, (((1,), (1,)), ((), ())), preferred_element_type=F32)

    def finish(masked):
        for i in range(len(pairs)):
            cols = slice(i * wide, (i + 1) * wide)
            z = z_ref[:, cols]
            if masked:
                col = step * blk + lax.broadcasted_iota(jnp.int32, z.shape, 0)
                z = jnp.where(col < limit_ref[0], z, -jnp.inf)
                z_ref[:, cols] = z
            old = stat_ref[k:k + 1, cols]
            new = jnp.maximum(old, jnp.max(z, axis=0, keepdims=True))
            total = jnp.sum(jnp.exp(z - new), axis=0, keepdims=True)
            stat_ref[k:k + 1, cols] = new
            stat_ref[4 + k:5 + k, cols] = stat_ref[4 + k:5 + k, cols] * jnp.exp(old - new) + total

    pl.when(step < steps - 1)(lambda: finish(False))
    pl.when(step == steps - 1)(lambda: finish(True))


def fwd_call(k, parts, wt, limit, stats):
    vocab, dim = wt.shape
    toks = sum(p.shape[0] for p in parts)
    blocks = pl.cdiv(vocab, BLK)
    assert vocab - (blocks - 1) * BLK > PAD_COLS
    return pl.pallas_call(
        functools.partial(fwd_body, k, len(parts), BLK),
        grid=(blocks,),
        in_specs=[pl.BlockSpec(memory_space=pltpu.SMEM), pl.BlockSpec((BLK, dim), lambda j: (j, 0))]
        + [whole(p.shape) for p in parts] + [whole((8, toks))] * len(stats),
        out_specs=[pl.BlockSpec((BLK, toks), lambda j: (j, 0)), whole((8, toks))],
        out_shape=[jax.ShapeDtypeStruct((vocab, toks), F32), jax.ShapeDtypeStruct((8, toks), F32)],
        compiler_params=params(1),
        cost_estimate=pl.CostEstimate(
            flops=2 * vocab * dim * toks, bytes_accessed=vocab * dim * 2 + vocab * toks * 4,
            transcendentals=vocab * toks),
        name="fwd",
    )(limit, wt, *parts, *stats)


TILE = 1024


def mix(first, keep_ref, got_ref, outs):
    q = keep_ref[...] + got_ref[...]
    dhalf = q.shape[1] // 2

    @pl.when(first)
    def _():
        outs[0][...], outs[1][...] = q[:, :dhalf], q[:, dhalf:]

    @pl.when(jnp.logical_not(first))
    def _():
        outs[2][...], outs[3][...] = q[:, :dhalf], q[:, dhalf:]


def back_body(k, mixing, blk, vocab, label_ref, lse_ref, scale_ref, loss_ref, z_ref, wt_ref, *refs):
    dz_ref, keep_ref, send_ref, lost_ref = refs[-10:-6] if mixing else refs[-6:-2]
    acc_ref, sem = refs[-2:]
    step, steps = pl.program_id(0), pl.num_programs(0)
    tail = vocab - (vocab // blk) * blk or blk
    rows, dim = keep_ref.shape
    row = slice(k, k + 1)

    @pl.when(step == 0)
    def _():
        acc_ref[...] = jnp.zeros_like(acc_ref)
        lost_ref[...] = loss_ref[...]

    if mixing:
        mix(step < steps // 2, refs[0], refs[1], refs[-6:-2])

    def run(size, leave):
        z = z_ref[:size]
        col = step * blk + lax.broadcasted_iota(jnp.int32, z.shape, 0)
        hit = col == label_ref[row]
        scale = scale_ref[row]
        dz = ((jnp.exp(z - lse_ref[row]) - jnp.where(hit, 1.0, 0.0)) * scale).astype(BF16)
        dz_ref[:size] = dz
        lost = jnp.sum(jnp.where(hit, z, 0.0), axis=0, keepdims=True) * scale
        wide = lost_ref.shape[1]
        lost_ref[0:1] = lost_ref[0:1] - sum(lost[:, i:i + wide] for i in range(0, lost.shape[1], wide))
        copies = []
        for t in range(dim // TILE):
            cols = slice(t * TILE, (t + 1) * TILE)
            acc_ref[:, cols] += lax.dot_general(
                dz, wt_ref[:size, cols], (((0,), (0,)), ((), ())), preferred_element_type=F32)
            if leave:
                for h, out in enumerate((keep_ref, send_ref)):
                    copies.append(pltpu.make_async_copy(
                        acc_ref.at[h * rows:(h + 1) * rows, cols], out.at[:, cols], sem.at[2 * t + h]))
                    copies[-1].start()
        for c in copies:
            c.wait()

    pl.when(step < steps - 1)(lambda: run(blk, False))
    pl.when(step == steps - 1)(lambda: run(tail, True))


def back_call(k, z, wt, label, lse, scale, loss, shared, pair):
    vocab, dim = wt.shape
    toks = z.shape[1]
    rows = toks // 2
    steps = pl.cdiv(vocab, BLK)
    mixing = bool(pair)
    in_specs = [whole((8, toks))] * 3 + [whole((8, 128)), pl.BlockSpec((BLK, toks), lambda j: (j, 0)),
                                         pl.BlockSpec((BLK, dim), lambda j: (j, 0))]
    out_specs = [pl.BlockSpec((BLK, toks), lambda j: (j, k)), ANY, ANY, whole((8, 128))]
    out_shape = [jax.ShapeDtypeStruct((vocab, 4 * toks), BF16), jax.ShapeDtypeStruct((rows, dim), F32),
                 jax.ShapeDtypeStruct((rows, dim), F32), jax.ShapeDtypeStruct((8, 128), F32)]
    if mixing:
        blk, mid, dhalf = rows // steps, steps // 2, dim // 2
        low = pl.BlockSpec((blk, dhalf), lambda j: (jnp.minimum(j, mid - 1), 0))
        high = pl.BlockSpec((blk, dhalf), lambda j: (jnp.maximum(j - mid, 0), 0))
        in_specs += [pl.BlockSpec((blk, dim), lambda j: (j, 0))] * 2
        out_specs += [low, low, high, high]
        out_shape += [jax.ShapeDtypeStruct((rows // 2, dhalf), F32)] * 4
    args = [label, lse, scale, loss, z, wt, *pair, *shared]
    return pl.pallas_call(
        functools.partial(back_body, k, mixing, BLK, vocab),
        grid=(steps,),
        in_specs=in_specs + [ANY] * len(shared),
        out_specs=out_specs,
        out_shape=out_shape,
        input_output_aliases={len(args) - 1: 0} if shared else {},
        scratch_shapes=[pltpu.VMEM((toks, dim), F32), pltpu.SemaphoreType.DMA((2 * dim // TILE,))],
        compiler_params=params(1),
        cost_estimate=pl.CostEstimate(
            flops=2 * vocab * dim * toks, bytes_accessed=vocab * dim * 2 + vocab * toks * 6,
            transcendentals=vocab * toks),
        name="back",
    )(*args)


def weight_body(n_parts, dz_ref, keep_ref, got_ref, *refs):
    a_refs, out_ref, q_ref = refs[:n_parts], refs[-2], refs[-1]
    q_ref[...] = keep_ref[...] + got_ref[...]

    @pl.loop(0, out_ref.shape[1] // TILE)
    def _(k):
        cols = pl.ds(pl.multiple_of(k * TILE, TILE), TILE)
        a = jnp.concatenate([r[:, cols] for r in a_refs], axis=0)
        out_ref[:, cols] = jnp.dot(dz_ref[...], a, preferred_element_type=F32)


def weight_call(dz, parts, keep, got):
    vocab, toks = dz.shape
    dim = parts[0].shape[1]
    rows, cols = 1024, dim // 2
    blocks = pl.cdiv(vocab, rows)
    share = pl.BlockSpec((keep.shape[0] // (blocks * (dim // cols)), dim), lambda n, j: (n * blocks + j, 0))
    return pl.pallas_call(
        functools.partial(weight_body, len(parts)),
        grid=(dim // cols, blocks),
        in_specs=[pl.BlockSpec((rows, toks), lambda n, j: (j, 0)), share, share]
        + [pl.BlockSpec((p.shape[0], cols), lambda n, j: (0, n)) for p in parts],
        out_specs=[pl.BlockSpec((rows, cols), lambda n, j: (j, n)), share],
        out_shape=[jax.ShapeDtypeStruct((vocab, dim), F32), jax.ShapeDtypeStruct(keep.shape, F32)],
        compiler_params=params(2),
        cost_estimate=pl.CostEstimate(
            flops=2 * vocab * dim * toks, bytes_accessed=vocab * dim * 4 + vocab * toks * 4, transcendentals=0),
        name="dweight",
    )(dz, keep, got, *parts)


def norm_body(hid_ref, gain_ref, lo_ref, hi_ref):
    step = pl.program_id(0)
    x = hid_ref[...].astype(F32)
    inv = lax.rsqrt(jnp.mean(x * x, axis=-1, keepdims=True) + NORM_EPS)
    a = (x * inv * gain_ref[...]).astype(BF16)

    @pl.when(step < pl.num_programs(0) // 2)
    def _():
        lo_ref[...] = a

    @pl.when(step >= pl.num_programs(0) // 2)
    def _():
        hi_ref[...] = a


def norm_call(hidden, gain, order):
    rows, dim = hidden.shape
    steps = 2
    blk, mid = rows // steps, steps // 2
    body = lambda *refs: norm_body(refs[0], refs[1], refs[-2], refs[-1])
    return pl.pallas_call(
        body,
        grid=(steps,),
        in_specs=[pl.BlockSpec((blk, dim), lambda i: (i, 0)), whole((1, dim))] + [ANY] * len(order),
        out_specs=[pl.BlockSpec((blk, dim), lambda i: (jnp.minimum(i, mid - 1), 0)),
                   pl.BlockSpec((blk, dim), lambda i: (jnp.maximum(i - mid, 0), 0))],
        out_shape=[jax.ShapeDtypeStruct((rows // 2, dim), BF16)] * 2,
        compiler_params=params(1),
        cost_estimate=pl.CostEstimate(flops=5 * rows * dim, bytes_accessed=rows * dim * 4, transcendentals=rows),
        name="norm",
    )(hidden, gain[None], *order)


def peer(me, mask):
    out = me
    for bit in (1, 2, 4):
        if mask & bit:
            out = out + bit * (1 - 2 * ((me // bit) % 2))
    return out


def push_all(n, sends, send_sem, recv_sem):
    me = lax.axis_index("vp")
    barrier = pltpu.get_barrier_semaphore()
    for m in range(1, n):
        pl.semaphore_signal(barrier, inc=1, device_id={"vp": peer(me, m)}, device_id_type=pl.DeviceIdType.MESH)
    pl.semaphore_wait(barrier, n - 1)
    copies = [
        pltpu.make_async_remote_copy(
            src_ref=src, dst_ref=got.at[m], send_sem=send_sem.at[i, m], recv_sem=recv_sem.at[i, m],
            device_id={"vp": peer(me, m)}, device_id_type=pl.DeviceIdType.MESH)
        for m in range(1, n) for i, (src, got) in enumerate(sends)
    ]
    for c in copies:
        c.start()
    for c in copies:
        c.wait()


def tree(v):
    while len(v) > 1:
        v = [v[i] + v[i + 1] for i in range(0, len(v), 2)]
    return v[0]


def sum_body(n, gain_ref, loss_ref, gain_out, loss_out, got_gain, got_loss, send_sem, recv_sem):
    push_all(n, [(gain_ref, got_gain), (loss_ref, got_loss)], send_sem, recv_sem)
    gain = tree([gain_ref[...]] + [got_gain[m] for m in range(1, n)])
    per = gain.shape[1] // 128
    for i in range(gain.shape[0]):
        for j in range(per):
            gain_out[i * per + j:i * per + j + 1] = gain[i:i + 1, j * 128:(j + 1) * 128]
    loss = tree([loss_ref[...]] + [got_loss[m] for m in range(1, n)])
    loss_out[...] = jnp.sum(loss[0:1], axis=1, keepdims=True)


LAYOUT = (
    ((0, 0), (0, 1), (1, 0), (1, 1)),
    ((2, 0), (4, 0), (3, 0), (5, 0)),
    ((2, 1), (4, 1), (3, 1), (5, 1)),
    ((6, 0), (6, 1), (7, 0), (7, 1)),
)


def stats_body(n, vocab, stat_ref, label_ref, weight_ref, label_out, lse_out, scale_out, loss_out,
               got_stat, got_label, got_weight, send_sem, recv_sem):
    push_all(n, [(stat_ref, got_stat), (label_ref, got_label), (weight_ref, got_weight)], send_sem, recv_sem)
    width = stat_ref.shape[1] // 4
    base = lax.axis_index("vp") * vocab
    place = {key: (k, i) for k, row in enumerate(LAYOUT) for i, key in enumerate(row)}
    pick = lambda own, got, m, *at: own[at] if m == 0 else got[(m,) + at]
    lanes = lambda i: slice(i * width, (i + 1) * width)
    one = lambda k: slice(k, k + 1)
    total_weight = tree([
        jnp.sum(pick(weight_ref, got_weight, m, slice(0, 2)), axis=(0, 1), keepdims=True) for m in range(n)])
    loss = jnp.zeros((1, width), F32)
    label_out[4:] = jnp.zeros((4, 4 * width), jnp.int32)
    lse_out[4:] = jnp.zeros((4, 4 * width), F32)
    scale_out[4:] = jnp.zeros((4, 4 * width), F32)
    for k, row in enumerate(LAYOUT):
        for i, (r, h) in enumerate(row):
            tops, sums = [], []
            for m in range(n):
                kk, ii = place[(r ^ m, h)]
                tops.append(pick(stat_ref, got_stat, m, one(kk), lanes(ii)))
                sums.append(pick(stat_ref, got_stat, m, one(4 + kk), lanes(ii)))
            top = functools.reduce(jnp.maximum, tops)
            lse = top + jnp.log(tree([s * jnp.exp(t - top) for s, t in zip(sums, tops)]))
            scale = pick(weight_ref, got_weight, r, one(h)) / total_weight
            lse_out[one(k), lanes(i)] = lse
            scale_out[one(k), lanes(i)] = scale
            label_out[one(k), lanes(i)] = pick(label_ref, got_label, r, one(h)) - base
            if r == 0:
                loss = loss + scale * lse
    loss_out[...] = jnp.zeros(loss_out.shape, F32)
    loss_out[0:1] = loss


def small_call(body, n, args, outs, ident):
    vm = pl.BlockSpec(memory_space=pltpu.VMEM)
    sems = [pltpu.SemaphoreType.DMA((len(args), n))] * 2
    return pl.pallas_call(
        body,
        in_specs=[vm] * len(args),
        out_specs=[vm] * len(outs),
        out_shape=outs,
        scratch_shapes=[pltpu.VMEM((n,) + v.shape, v.dtype) for v in args] + sems,
        compiler_params=pltpu.CompilerParams(collective_id=ident, has_side_effects=True),
        cost_estimate=pl.CostEstimate(flops=4000, bytes_accessed=4_000_000, transcendentals=0),
    )(*args)


def mix_body(keep_ref, got_ref, a_ref, b_ref):
    q = keep_ref[...] + got_ref[...]
    dhalf = q.shape[1] // 2
    a_ref[...], b_ref[...] = q[:, :dhalf], q[:, dhalf:]


def mix_call(keep, got):
    rows, dim = keep.shape
    steps = 4
    blk, dhalf = rows // steps, dim // 2
    full = pl.BlockSpec((blk, dim), lambda i: (i, 0))
    return pl.pallas_call(
        mix_body,
        grid=(steps,),
        in_specs=[full, full],
        out_specs=[pl.BlockSpec((blk, dhalf), lambda i: (i, 0))] * 2,
        out_shape=[jax.ShapeDtypeStruct((rows, dhalf), F32)] * 2,
        compiler_params=params(1),
        cost_estimate=pl.CostEstimate(flops=rows * dim, bytes_accessed=rows * dim * 12, transcendentals=0),
        name="mix",
    )(keep, got)


def second_body(keep2_ref, keep4_ref, got2_ref, got4_ref, sa_ref, ta_ref, xa_ref, xb_ref, ya_ref, yb_ref,
                x2_ref, y4_ref, s_ref, t_ref):
    dhalf = sa_ref.shape[1]
    q2 = keep2_ref[...] + got2_ref[...]
    q4 = keep4_ref[...] + got4_ref[...]
    x2_ref[...] = q2[:, :dhalf]
    y4_ref[...] = q4[:, dhalf:]
    s_ref[0] = sa_ref[...] + xa_ref[...]
    s_ref[1] = q4[:, :dhalf] + xb_ref[...]
    t_ref[0] = ta_ref[...] + ya_ref[...]
    t_ref[1] = q2[:, dhalf:] + yb_ref[...]


def second_call(keep, got, sa, ta, x, y):
    half, dhalf = sa.shape
    steps = 4
    blk = half // steps
    at = lambda width, off: pl.BlockSpec((blk, width), lambda i: (i + off, 0))
    two = pl.BlockSpec((2, blk, dhalf), lambda i: (0, i, 0))
    return pl.pallas_call(
        second_body,
        grid=(steps,),
        in_specs=[at(2 * dhalf, 0), at(2 * dhalf, steps), at(2 * dhalf, 0), at(2 * dhalf, steps), at(dhalf, 0), at(dhalf, 0),
                  at(dhalf, 0), at(dhalf, steps), at(dhalf, 0), at(dhalf, steps)],
        out_specs=[at(dhalf, 0), at(dhalf, 0), two, two],
        out_shape=[jax.ShapeDtypeStruct((half, dhalf), F32)] * 2 + [jax.ShapeDtypeStruct((2, half, dhalf), F32)] * 2,
        compiler_params=params(1),
        cost_estimate=pl.CostEstimate(flops=8 * half * dhalf, bytes_accessed=half * dhalf * 80, transcendentals=0),
        name="second",
    )(keep, keep, got, got, sa, ta, x, x, y, y)


def last_body(hid_ref, gain_ref, q_ref, x2a_ref, x2b_ref, s4_ref, y4a_ref, y4b_ref, t2_ref, dh_ref, dgain_ref):
    step = pl.program_id(0)
    dhalf = s4_ref.shape[1]

    def run(x2_ref, y4_ref):
        q = q_ref[...]
        g = jnp.concatenate(
            [q[:, :dhalf] + x2_ref[...] + s4_ref[...], q[:, dhalf:] + y4_ref[...] + t2_ref[...]], axis=1)
        x = hid_ref[...].astype(F32)
        inv = lax.rsqrt(jnp.mean(x * x, axis=-1, keepdims=True) + NORM_EPS)
        norm = x * inv
        u = g * gain_ref[...]
        dh_ref[...] = (inv * (u - norm * jnp.mean(u * norm, axis=-1, keepdims=True))).astype(BF16)
        part = jnp.sum(g * norm, axis=0, keepdims=True)
        wide = dgain_ref.shape[1]
        for k in range(dgain_ref.shape[0]):
            piece = part[:, k * wide:(k + 1) * wide]
            dgain_ref[k:k + 1] = jnp.where(step == 0, piece, dgain_ref[k:k + 1] + piece)

    pl.when(step < pl.num_programs(0) // 2)(lambda: run(x2a_ref, y4a_ref))
    pl.when(step >= pl.num_programs(0) // 2)(lambda: run(x2b_ref, y4b_ref))


def last_call(hidden, gain, q, x2a, x2b, s4, y4a, y4b, t2):
    rows, dim = hidden.shape
    steps = 4
    blk, mid, dhalf = rows // steps, steps // 2, dim // 2
    row = lambda width: pl.BlockSpec((blk, width), lambda i: (i, 0))
    low = pl.BlockSpec((blk, dhalf), lambda i: (jnp.minimum(i, mid - 1), 0))
    high = pl.BlockSpec((blk, dhalf), lambda i: (jnp.maximum(i - mid, 0), 0))
    return pl.pallas_call(
        last_body,
        grid=(steps,),
        in_specs=[row(dim), whole((1, dim)), row(dim), low, high, row(dhalf), low, high, row(dhalf)],
        out_specs=[row(dim), whole((8, dim // 8))],
        out_shape=[jax.ShapeDtypeStruct((rows, dim), BF16), jax.ShapeDtypeStruct((8, dim // 8), F32)],
        compiler_params=params(1),
        cost_estimate=pl.CostEstimate(flops=20 * rows * dim, bytes_accessed=rows * dim * 20, transcendentals=rows),
        name="last",
    )(hidden, gain[None], q, x2a, x2b, s4, y4a, y4b, t2)


def solution(mesh):
    n = mesh.shape["vp"]

    def swap(v, mask):
        return lax.ppermute(v, "vp", [(i, i ^ mask) for i in range(n)])

    def compute(hidden, labels, loss_weight, norm_gain, w_local):
        rows, dim = hidden.shape
        half, dhalf = rows // 2, dim // 2
        wt = w_local.T
        vocab_local = wt.shape[0]
        vocab_real = vocab_local * n - PAD_COLS
        me = lax.axis_index("vp")

        limit = jnp.minimum(vocab_real - me * vocab_local, vocab_local).astype(jnp.int32).reshape(1)

        r0a, r0b = norm_call(hidden, norm_gain, [])
        r2a, r4a = swap(r0a, 2), swap(r0a, 4)
        r1a, r1b = swap(r0a, 1), swap(r0b, 1)
        r2b, r4b = swap(r0b, 2), swap(r0b, 4)
        r3a, r5a = swap(r2a, 1), swap(r4a, 1)
        r3b, r5b = swap(r2b, 1), swap(r4b, 1)
        r6a, r6b = swap(r2a, 4), swap(r4b, 2)
        r7a, r7b = swap(r6a, 1), swap(r6b, 1)
        groups = [[r0a, r0b, r1a, r1b], [r2a, r4a, r3a, r5a], [r2b, r4b, r3b, r5b], [r6a, r6b, r7a, r7b]]

        logits_g, stats = [], []
        for k, parts in enumerate(groups):
            logits, stat = fwd_call(k, parts, wt, limit, stats)
            logits_g.append(logits)
            stats = [stat]

        spec = jax.ShapeDtypeStruct
        label, lse, scale, loss = small_call(
            functools.partial(stats_body, n, vocab_local), n,
            [stats[0], labels.reshape(2, half), loss_weight.reshape(2, half)],
            [spec((8, 2 * rows), jnp.int32), spec((8, 2 * rows), F32), spec((8, 2 * rows), F32), spec((8, half), F32)],
            0)

        def back(k, loss, shared, pair):
            return back_call(k, logits_g[k], wt, label, lse, scale, loss, shared, pair)

        dz, keep3, send3, loss = back(3, loss, [], [])
        got3 = swap(send3, 1)
        dz, keep1, send1, loss = back(1, loss, [dz], [])
        q6x, q6y = mix_call(keep3, got3)
        x6, y6 = swap(q6x, 2), swap(q6y, 4)
        got1 = swap(send1, 1)
        dz, keep2, send2, loss = back(2, loss, [dz], [])
        got2 = swap(send2, 1)
        dz, keep0, send0, loss, x2a, ta, sa, y4a = back(0, loss, [dz], [keep1, got1])
        x2a, y4a = swap(x2a, 2), swap(y4a, 4)
        got0 = swap(send0, 1)
        x2b, y4b, s4, t2 = second_call(keep2, got2, sa, ta, x6, y6)
        x2b, y4b = swap(x2b, 2), swap(y4b, 4)
        s4, t2 = swap(s4, 4).reshape(rows, dhalf), swap(t2, 2).reshape(rows, dhalf)

        dwt, q0 = weight_call(dz, [p for g in groups for p in g], keep0, got0)
        d_input, d_gain = last_call(hidden, norm_gain, q0, x2a, x2b, s4, y4a, y4b, t2)
        d_gain, loss = small_call(
            functools.partial(sum_body, n), n, [d_gain, loss], [spec((dim // 128, 128), F32), spec((1, 1), F32)], 1)
        return loss.reshape(1), d_input, dwt.T, d_gain.reshape(dim)

    return jax.shard_map(
        compute,
        mesh=mesh,
        in_specs=(P(("dp", "vp"), None), P(("dp", "vp")), P(("dp", "vp")), P(None), P(None, "vp")),
        out_specs=(P("dp"), P(("dp", "vp"), None), P("dp", "vp"), P("dp")),
        check_vma=False,
    )
```

```python
import functools

import jax
import jax.numpy as jnp
from jax import lax
from jax.experimental import pallas as pl
from jax.experimental.pallas import tpu as pltpu
from jax.sharding import PartitionSpec as P


NORM_EPS = 1e-5
PAD_COLS = 128
BLK = 512
BACK_BLK = 1024
VMEM = 67_043_328
F32 = jnp.float32
BF16 = jnp.bfloat16


ANY = pl.BlockSpec(memory_space=pl.ANY)


def whole(shape):
    return pl.BlockSpec(shape, lambda *_: (0,) * len(shape))


def params(n_axes):
    return pltpu.CompilerParams(
        dimension_semantics=("arbitrary",) * n_axes, vmem_limit_bytes=VMEM)


LOWEST = -3.4028234663852886e38


def fwd_body(k, n_parts, blk, limit_ref, wt_ref, *refs):
    a_refs = refs[:n_parts]
    z_ref, stat_ref, hold_ref = refs[-3:]
    step, steps = pl.program_id(0), pl.num_programs(0)
    pairs = [a_refs[i:i + 2] for i in range(0, n_parts, 2)]
    wide = 2 * a_refs[0].shape[0]

    def dots():
        for i, (lo, hi) in enumerate(pairs):
            a = jnp.concatenate([lo[...], hi[...]], axis=0)
            hold_ref[:, i * wide:(i + 1) * wide] = lax.dot_general(
                wt_ref[...], a, (((1,), (1,)), ((), ())), preferred_element_type=F32)

    def finish(masked):
        for i in range(len(pairs)):
            cols = slice(i * wide, (i + 1) * wide)
            z = hold_ref[:, cols]
            if masked:
                col = (step - 1) * blk + lax.broadcasted_iota(jnp.int32, z.shape, 0)
                z = jnp.where(col < limit_ref[0], z, -jnp.inf)
            z_ref[:, cols] = z
            old = stat_ref[k:k + 1, cols]
            new = jnp.maximum(old, jnp.max(z, axis=0, keepdims=True))
            total = jnp.sum(jnp.exp(z - new), axis=0, keepdims=True)
            stat_ref[k:k + 1, cols] = new
            stat_ref[4 + k:5 + k, cols] = stat_ref[4 + k:5 + k, cols] * jnp.exp(old - new) + total

    @pl.when(step == 0)
    def _():
        stat_ref[...] = jnp.zeros(stat_ref.shape, F32) if k == 0 else refs[n_parts][...]
        stat_ref[k:k + 1, :] = jnp.full((1, stat_ref.shape[1]), LOWEST, F32)
        stat_ref[4 + k:5 + k, :] = jnp.zeros((1, stat_ref.shape[1]), F32)
        dots()

    @pl.when((step > 0) & (step < steps - 1))
    def _():
        finish(False)
        dots()

    pl.when(step == steps - 1)(lambda: finish(True))


def fwd_call(k, parts, wt, limit, stats):
    vocab, dim = wt.shape
    toks = sum(p.shape[0] for p in parts)
    blocks = pl.cdiv(vocab, BLK)
    assert vocab - (blocks - 1) * BLK > PAD_COLS
    return pl.pallas_call(
        functools.partial(fwd_body, k, len(parts), BLK),
        grid=(blocks + 1,),
        in_specs=[pl.BlockSpec(memory_space=pltpu.SMEM), pl.BlockSpec((BLK, dim), lambda j: (jnp.minimum(j, blocks - 1), 0))]
        + [whole(p.shape) for p in parts] + [whole((8, toks))] * len(stats),
        out_specs=[pl.BlockSpec((BLK, toks), lambda j: (jnp.maximum(j - 1, 0), 0)), whole((8, toks))],
        out_shape=[jax.ShapeDtypeStruct((vocab, toks), F32), jax.ShapeDtypeStruct((8, toks), F32)],
        scratch_shapes=[pltpu.VMEM((BLK, toks), F32)],
        compiler_params=params(1),
        cost_estimate=pl.CostEstimate(
            flops=2 * vocab * dim * toks, bytes_accessed=vocab * dim * 2 + vocab * toks * 4,
            transcendentals=vocab * toks),
        name="fwd",
    )(limit, wt, *parts, *stats)


TILE = 1024


def mix(first, keep_ref, got_ref, outs):
    q = keep_ref[...] + got_ref[...]
    dhalf = q.shape[1] // 2

    @pl.when(first)
    def _():
        outs[0][...], outs[1][...] = q[:, :dhalf], q[:, dhalf:]

    @pl.when(jnp.logical_not(first))
    def _():
        outs[2][...], outs[3][...] = q[:, :dhalf], q[:, dhalf:]


def back_body(k, mixing, blk, vocab, label_ref, lse_ref, scale_ref, loss_ref, z_ref, wt_ref, *refs):
    dz_ref, keep_ref, send_ref, lost_ref = refs[-10:-6] if mixing else refs[-6:-2]
    acc_ref, sem = refs[-2:]
    step, steps = pl.program_id(0), pl.num_programs(0)
    tail = vocab - (vocab // blk) * blk or blk
    rows, dim = keep_ref.shape
    row = slice(k, k + 1)

    @pl.when(step == 0)
    def _():
        acc_ref[...] = jnp.zeros_like(acc_ref)
        lost_ref[...] = loss_ref[...]

    if mixing:
        mix(step < steps // 2, refs[0], refs[1], refs[-6:-2])

    def run(size, leave):
        z = z_ref[:size]
        col = step * blk + lax.broadcasted_iota(jnp.int32, z.shape, 0)
        hit = col == label_ref[row]
        scale = scale_ref[row]
        dz = ((jnp.exp(z - lse_ref[row]) - jnp.where(hit, 1.0, 0.0)) * scale).astype(BF16)
        dz_ref[:size] = dz
        lost = jnp.sum(jnp.where(hit, z, 0.0), axis=0, keepdims=True) * scale
        wide = lost_ref.shape[1]
        lost_ref[0:1] = lost_ref[0:1] - sum(lost[:, i:i + wide] for i in range(0, lost.shape[1], wide))
        copies = []
        for t in range(dim // TILE):
            cols = slice(t * TILE, (t + 1) * TILE)
            acc_ref[:, cols] += lax.dot_general(
                dz, wt_ref[:size, cols], (((0,), (0,)), ((), ())), preferred_element_type=F32)
            if leave:
                for h, out in enumerate((keep_ref, send_ref)):
                    copies.append(pltpu.make_async_copy(
                        acc_ref.at[h * rows:(h + 1) * rows, cols], out.at[:, cols], sem.at[2 * t + h]))
                    copies[-1].start()
        for c in copies:
            c.wait()

    pl.when(step < steps - 1)(lambda: run(blk, False))
    pl.when(step == steps - 1)(lambda: run(tail, True))


def back_call(k, z, wt, label, lse, scale, loss, shared, pair):
    vocab, dim = wt.shape
    toks = z.shape[1]
    rows = toks // 2
    steps = pl.cdiv(vocab, BACK_BLK)
    mixing = bool(pair)
    in_specs = [whole((8, toks))] * 3 + [whole((8, 128)), pl.BlockSpec((BACK_BLK, toks), lambda j: (j, 0)),
                                         pl.BlockSpec((BACK_BLK, dim), lambda j: (j, 0))]
    out_specs = [pl.BlockSpec((BACK_BLK, toks), lambda j: (j, k)), ANY, ANY, whole((8, 128))]
    out_shape = [jax.ShapeDtypeStruct((vocab, 4 * toks), BF16), jax.ShapeDtypeStruct((rows, dim), F32),
                 jax.ShapeDtypeStruct((rows, dim), F32), jax.ShapeDtypeStruct((8, 128), F32)]
    if mixing:
        blk, mid, dhalf = rows // steps, steps // 2, dim // 2
        low = pl.BlockSpec((blk, dhalf), lambda j: (jnp.minimum(j, mid - 1), 0))
        high = pl.BlockSpec((blk, dhalf), lambda j: (jnp.maximum(j - mid, 0), 0))
        in_specs += [pl.BlockSpec((blk, dim), lambda j: (j, 0))] * 2
        out_specs += [low, low, high, high]
        out_shape += [jax.ShapeDtypeStruct((rows // 2, dhalf), F32)] * 4
    args = [label, lse, scale, loss, z, wt, *pair, *shared]
    return pl.pallas_call(
        functools.partial(back_body, k, mixing, BACK_BLK, vocab),
        grid=(steps,),
        in_specs=in_specs + [ANY] * len(shared),
        out_specs=out_specs,
        out_shape=out_shape,
        input_output_aliases={len(args) - 1: 0} if shared else {},
        scratch_shapes=[pltpu.VMEM((toks, dim), F32), pltpu.SemaphoreType.DMA((2 * dim // TILE,))],
        compiler_params=params(1),
        cost_estimate=pl.CostEstimate(
            flops=2 * vocab * dim * toks, bytes_accessed=vocab * dim * 2 + vocab * toks * 6,
            transcendentals=vocab * toks),
        name="back",
    )(*args)


def weight_body(n_parts, dz_ref, keep_ref, got_ref, *refs):
    a_refs, out_ref, q_ref = refs[:n_parts], refs[-2], refs[-1]
    q_ref[...] = keep_ref[...] + got_ref[...]

    @pl.loop(0, out_ref.shape[1] // TILE)
    def _(k):
        cols = pl.ds(pl.multiple_of(k * TILE, TILE), TILE)
        a = jnp.concatenate([r[:, cols] for r in a_refs], axis=0)
        out_ref[:, cols] = jnp.dot(dz_ref[...], a, preferred_element_type=F32)


def weight_call(dz, parts, keep, got):
    vocab, toks = dz.shape
    dim = parts[0].shape[1]
    rows, cols = 1024, dim // 2
    blocks = pl.cdiv(vocab, rows)
    share = pl.BlockSpec((keep.shape[0] // (blocks * (dim // cols)), dim), lambda n, j: (n * blocks + j, 0))
    return pl.pallas_call(
        functools.partial(weight_body, len(parts)),
        grid=(dim // cols, blocks),
        in_specs=[pl.BlockSpec((rows, toks), lambda n, j: (j, 0)), share, share]
        + [pl.BlockSpec((p.shape[0], cols), lambda n, j: (0, n)) for p in parts],
        out_specs=[pl.BlockSpec((rows, cols), lambda n, j: (j, n)), share],
        out_shape=[jax.ShapeDtypeStruct((vocab, dim), F32), jax.ShapeDtypeStruct(keep.shape, F32)],
        compiler_params=params(2),
        cost_estimate=pl.CostEstimate(
            flops=2 * vocab * dim * toks, bytes_accessed=vocab * dim * 4 + vocab * toks * 4, transcendentals=0),
        name="dweight",
    )(dz, keep, got, *parts)


def norm_body(hid_ref, gain_ref, lo_ref, hi_ref):
    step = pl.program_id(0)
    x = hid_ref[...].astype(F32)
    inv = lax.rsqrt(jnp.mean(x * x, axis=-1, keepdims=True) + NORM_EPS)
    a = (x * inv * gain_ref[...]).astype(BF16)

    @pl.when(step < pl.num_programs(0) // 2)
    def _():
        lo_ref[...] = a

    @pl.when(step >= pl.num_programs(0) // 2)
    def _():
        hi_ref[...] = a


def norm_call(hidden, gain, order):
    rows, dim = hidden.shape
    steps = 2
    blk, mid = rows // steps, steps // 2
    body = lambda *refs: norm_body(refs[0], refs[1], refs[-2], refs[-1])
    return pl.pallas_call(
        body,
        grid=(steps,),
        in_specs=[pl.BlockSpec((blk, dim), lambda i: (i, 0)), whole((1, dim))] + [ANY] * len(order),
        out_specs=[pl.BlockSpec((blk, dim), lambda i: (jnp.minimum(i, mid - 1), 0)),
                   pl.BlockSpec((blk, dim), lambda i: (jnp.maximum(i - mid, 0), 0))],
        out_shape=[jax.ShapeDtypeStruct((rows // 2, dim), BF16)] * 2,
        compiler_params=params(1),
        cost_estimate=pl.CostEstimate(flops=5 * rows * dim, bytes_accessed=rows * dim * 4, transcendentals=rows),
        name="norm",
    )(hidden, gain[None], *order)


def peer(me, mask):
    out = me
    for bit in (1, 2, 4):
        if mask & bit:
            out = out + bit * (1 - 2 * ((me // bit) % 2))
    return out


def push_all(n, sends, send_sem, recv_sem):
    me = lax.axis_index("vp")
    barrier = pltpu.get_barrier_semaphore()
    for m in range(1, n):
        pl.semaphore_signal(barrier, inc=1, device_id={"vp": peer(me, m)}, device_id_type=pl.DeviceIdType.MESH)
    pl.semaphore_wait(barrier, n - 1)
    copies = [
        pltpu.make_async_remote_copy(
            src_ref=src, dst_ref=got.at[m], send_sem=send_sem.at[i, m], recv_sem=recv_sem.at[i, m],
            device_id={"vp": peer(me, m)}, device_id_type=pl.DeviceIdType.MESH)
        for m in range(1, n) for i, (src, got) in enumerate(sends)
    ]
    for c in copies:
        c.start()
    for c in copies:
        c.wait()


def tree(v):
    while len(v) > 1:
        v = [v[i] + v[i + 1] for i in range(0, len(v), 2)]
    return v[0]


def sum_body(n, gain_ref, loss_ref, gain_out, loss_out, got_gain, got_loss, send_sem, recv_sem):
    push_all(n, [(gain_ref, got_gain), (loss_ref, got_loss)], send_sem, recv_sem)
    gain = tree([gain_ref[...]] + [got_gain[m] for m in range(1, n)])
    per = gain.shape[1] // 128
    for i in range(gain.shape[0]):
        for j in range(per):
            gain_out[i * per + j:i * per + j + 1] = gain[i:i + 1, j * 128:(j + 1) * 128]
    loss = tree([loss_ref[...]] + [got_loss[m] for m in range(1, n)])
    loss_out[...] = jnp.sum(loss[0:1], axis=1, keepdims=True)


LAYOUT = (
    ((0, 0), (0, 1), (1, 0), (1, 1)),
    ((2, 0), (4, 0), (3, 0), (5, 0)),
    ((2, 1), (4, 1), (3, 1), (5, 1)),
    ((6, 0), (6, 1), (7, 0), (7, 1)),
)


def stats_body(n, vocab, stat_ref, label_ref, weight_ref, label_out, lse_out, scale_out, loss_out,
               got_stat, got_label, got_weight, send_sem, recv_sem):
    push_all(n, [(stat_ref, got_stat), (label_ref, got_label), (weight_ref, got_weight)], send_sem, recv_sem)
    width = stat_ref.shape[1] // 4
    base = lax.axis_index("vp") * vocab
    place = {key: (k, i) for k, row in enumerate(LAYOUT) for i, key in enumerate(row)}
    pick = lambda own, got, m, *at: own[at] if m == 0 else got[(m,) + at]
    lanes = lambda i: slice(i * width, (i + 1) * width)
    one = lambda k: slice(k, k + 1)
    total_weight = tree([
        jnp.sum(pick(weight_ref, got_weight, m, slice(0, 2)), axis=(0, 1), keepdims=True) for m in range(n)])
    loss = jnp.zeros((1, width), F32)
    label_out[4:] = jnp.zeros((4, 4 * width), jnp.int32)
    lse_out[4:] = jnp.zeros((4, 4 * width), F32)
    scale_out[4:] = jnp.zeros((4, 4 * width), F32)
    for k, row in enumerate(LAYOUT):
        for i, (r, h) in enumerate(row):
            tops, sums = [], []
            for m in range(n):
                kk, ii = place[(r ^ m, h)]
                tops.append(pick(stat_ref, got_stat, m, one(kk), lanes(ii)))
                sums.append(pick(stat_ref, got_stat, m, one(4 + kk), lanes(ii)))
            top = functools.reduce(jnp.maximum, tops)
            lse = top + jnp.log(tree([s * jnp.exp(t - top) for s, t in zip(sums, tops)]))
            scale = pick(weight_ref, got_weight, r, one(h)) / total_weight
            lse_out[one(k), lanes(i)] = lse
            scale_out[one(k), lanes(i)] = scale
            label_out[one(k), lanes(i)] = pick(label_ref, got_label, r, one(h)) - base
            if r == 0:
                loss = loss + scale * lse
    loss_out[...] = jnp.zeros(loss_out.shape, F32)
    loss_out[0:1] = loss


def small_call(body, n, args, outs, ident):
    vm = pl.BlockSpec(memory_space=pltpu.VMEM)
    sems = [pltpu.SemaphoreType.DMA((len(args), n))] * 2
    return pl.pallas_call(
        body,
        in_specs=[vm] * len(args),
        out_specs=[vm] * len(outs),
        out_shape=outs,
        scratch_shapes=[pltpu.VMEM((n,) + v.shape, v.dtype) for v in args] + sems,
        compiler_params=pltpu.CompilerParams(collective_id=ident, has_side_effects=True),
        cost_estimate=pl.CostEstimate(flops=4000, bytes_accessed=4_000_000, transcendentals=0),
    )(*args)


def mix_body(keep_ref, got_ref, a_ref, b_ref):
    q = keep_ref[...] + got_ref[...]
    dhalf = q.shape[1] // 2
    a_ref[...], b_ref[...] = q[:, :dhalf], q[:, dhalf:]


def mix_call(keep, got):
    rows, dim = keep.shape
    steps = 4
    blk, dhalf = rows // steps, dim // 2
    full = pl.BlockSpec((blk, dim), lambda i: (i, 0))
    return pl.pallas_call(
        mix_body,
        grid=(steps,),
        in_specs=[full, full],
        out_specs=[pl.BlockSpec((blk, dhalf), lambda i: (i, 0))] * 2,
        out_shape=[jax.ShapeDtypeStruct((rows, dhalf), F32)] * 2,
        compiler_params=params(1),
        cost_estimate=pl.CostEstimate(flops=rows * dim, bytes_accessed=rows * dim * 12, transcendentals=0),
        name="mix",
    )(keep, got)


def second_body(keep2_ref, keep4_ref, got2_ref, got4_ref, sa_ref, ta_ref, xa_ref, xb_ref, ya_ref, yb_ref,
                x2_ref, y4_ref, s_ref, t_ref):
    dhalf = sa_ref.shape[1]
    q2 = keep2_ref[...] + got2_ref[...]
    q4 = keep4_ref[...] + got4_ref[...]
    x2_ref[...] = q2[:, :dhalf]
    y4_ref[...] = q4[:, dhalf:]
    s_ref[0] = sa_ref[...] + xa_ref[...]
    s_ref[1] = q4[:, :dhalf] + xb_ref[...]
    t_ref[0] = ta_ref[...] + ya_ref[...]
    t_ref[1] = q2[:, dhalf:] + yb_ref[...]


def second_call(keep, got, sa, ta, x, y):
    half, dhalf = sa.shape
    steps = 4
    blk = half // steps
    at = lambda width, off: pl.BlockSpec((blk, width), lambda i: (i + off, 0))
    two = pl.BlockSpec((2, blk, dhalf), lambda i: (0, i, 0))
    return pl.pallas_call(
        second_body,
        grid=(steps,),
        in_specs=[at(2 * dhalf, 0), at(2 * dhalf, steps), at(2 * dhalf, 0), at(2 * dhalf, steps), at(dhalf, 0), at(dhalf, 0),
                  at(dhalf, 0), at(dhalf, steps), at(dhalf, 0), at(dhalf, steps)],
        out_specs=[at(dhalf, 0), at(dhalf, 0), two, two],
        out_shape=[jax.ShapeDtypeStruct((half, dhalf), F32)] * 2 + [jax.ShapeDtypeStruct((2, half, dhalf), F32)] * 2,
        compiler_params=params(1),
        cost_estimate=pl.CostEstimate(flops=8 * half * dhalf, bytes_accessed=half * dhalf * 80, transcendentals=0),
        name="second",
    )(keep, keep, got, got, sa, ta, x, x, y, y)


def last_body(hid_ref, gain_ref, q_ref, x2a_ref, x2b_ref, s4_ref, y4a_ref, y4b_ref, t2_ref, dh_ref, dgain_ref):
    step = pl.program_id(0)
    dhalf = s4_ref.shape[1]

    def run(x2_ref, y4_ref):
        q = q_ref[...]
        g = jnp.concatenate(
            [q[:, :dhalf] + x2_ref[...] + s4_ref[...], q[:, dhalf:] + y4_ref[...] + t2_ref[...]], axis=1)
        x = hid_ref[...].astype(F32)
        inv = lax.rsqrt(jnp.mean(x * x, axis=-1, keepdims=True) + NORM_EPS)
        norm = x * inv
        u = g * gain_ref[...]
        dh_ref[...] = (inv * (u - norm * jnp.mean(u * norm, axis=-1, keepdims=True))).astype(BF16)
        part = jnp.sum(g * norm, axis=0, keepdims=True)
        wide = dgain_ref.shape[1]
        for k in range(dgain_ref.shape[0]):
            piece = part[:, k * wide:(k + 1) * wide]
            dgain_ref[k:k + 1] = jnp.where(step == 0, piece, dgain_ref[k:k + 1] + piece)

    pl.when(step < pl.num_programs(0) // 2)(lambda: run(x2a_ref, y4a_ref))
    pl.when(step >= pl.num_programs(0) // 2)(lambda: run(x2b_ref, y4b_ref))


def last_call(hidden, gain, q, x2a, x2b, s4, y4a, y4b, t2):
    rows, dim = hidden.shape
    steps = 4
    blk, mid, dhalf = rows // steps, steps // 2, dim // 2
    row = lambda width: pl.BlockSpec((blk, width), lambda i: (i, 0))
    low = pl.BlockSpec((blk, dhalf), lambda i: (jnp.minimum(i, mid - 1), 0))
    high = pl.BlockSpec((blk, dhalf), lambda i: (jnp.maximum(i - mid, 0), 0))
    return pl.pallas_call(
        last_body,
        grid=(steps,),
        in_specs=[row(dim), whole((1, dim)), row(dim), low, high, row(dhalf), low, high, row(dhalf)],
        out_specs=[row(dim), whole((8, dim // 8))],
        out_shape=[jax.ShapeDtypeStruct((rows, dim), BF16), jax.ShapeDtypeStruct((8, dim // 8), F32)],
        compiler_params=params(1),
        cost_estimate=pl.CostEstimate(flops=20 * rows * dim, bytes_accessed=rows * dim * 20, transcendentals=rows),
        name="last",
    )(hidden, gain[None], q, x2a, x2b, s4, y4a, y4b, t2)


def solution(mesh):
    n = mesh.shape["vp"]

    def swap(v, mask):
        return lax.ppermute(v, "vp", [(i, i ^ mask) for i in range(n)])

    def compute(hidden, labels, loss_weight, norm_gain, w_local):
        rows, dim = hidden.shape
        half, dhalf = rows // 2, dim // 2
        wt = w_local.T
        vocab_local = wt.shape[0]
        vocab_real = vocab_local * n - PAD_COLS
        me = lax.axis_index("vp")

        limit = jnp.minimum(vocab_real - me * vocab_local, vocab_local).astype(jnp.int32).reshape(1)

        r0a, r0b = norm_call(hidden, norm_gain, [])
        r2a, r4a = swap(r0a, 2), swap(r0a, 4)
        r1a, r1b = swap(r0a, 1), swap(r0b, 1)
        r2b, r4b = swap(r0b, 2), swap(r0b, 4)
        r3a, r5a = swap(r2a, 1), swap(r4a, 1)
        r3b, r5b = swap(r2b, 1), swap(r4b, 1)
        r6a, r6b = swap(r2a, 4), swap(r4b, 2)
        r7a, r7b = swap(r6a, 1), swap(r6b, 1)
        groups = [[r0a, r0b, r1a, r1b], [r2a, r4a, r3a, r5a], [r2b, r4b, r3b, r5b], [r6a, r6b, r7a, r7b]]

        logits_g, stats = [], []
        for k, parts in enumerate(groups):
            logits, stat = fwd_call(k, parts, wt, limit, stats)
            logits_g.append(logits)
            stats = [stat]

        spec = jax.ShapeDtypeStruct
        label, lse, scale, loss = small_call(
            functools.partial(stats_body, n, vocab_local), n,
            [stats[0], labels.reshape(2, half), loss_weight.reshape(2, half)],
            [spec((8, 2 * rows), jnp.int32), spec((8, 2 * rows), F32), spec((8, 2 * rows), F32), spec((8, half), F32)],
            0)

        def back(k, loss, shared, pair):
            return back_call(k, logits_g[k], wt, label, lse, scale, loss, shared, pair)

        dz, keep3, send3, loss = back(3, loss, [], [])
        got3 = swap(send3, 1)
        dz, keep1, send1, loss = back(1, loss, [dz], [])
        q6x, q6y = mix_call(keep3, got3)
        x6, y6 = swap(q6x, 2), swap(q6y, 4)
        got1 = swap(send1, 1)
        dz, keep2, send2, loss = back(2, loss, [dz], [])
        got2 = swap(send2, 1)
        dz, keep0, send0, loss, x2a, ta, sa, y4a = back(0, loss, [dz], [keep1, got1])
        x2a, y4a = swap(x2a, 2), swap(y4a, 4)
        got0 = swap(send0, 1)
        x2b, y4b, s4, t2 = second_call(keep2, got2, sa, ta, x6, y6)
        x2b, y4b = swap(x2b, 2), swap(y4b, 4)
        s4, t2 = swap(s4, 4).reshape(rows, dhalf), swap(t2, 2).reshape(rows, dhalf)

        dwt, q0 = weight_call(dz, [p for g in groups for p in g], keep0, got0)
        d_input, d_gain = last_call(hidden, norm_gain, q0, x2a, x2b, s4, y4a, y4b, t2)
        d_gain, loss = small_call(
            functools.partial(sum_body, n), n, [d_gain, loss], [spec((dim // 128, 128), F32), spec((1, 1), F32)], 1)
        return loss.reshape(1), d_input, dwt.T, d_gain.reshape(dim)

    return jax.shard_map(
        compute,
        mesh=mesh,
        in_specs=(P(("dp", "vp"), None), P(("dp", "vp")), P(("dp", "vp")), P(None), P(None, "vp")),
        out_specs=(P("dp"), P(("dp", "vp"), None), P("dp", "vp"), P("dp")),
        check_vma=False,
    )
```

```python
import functools

import jax
import jax.numpy as jnp
from jax import lax
from jax.experimental import pallas as pl
from jax.experimental.pallas import tpu as pltpu
from jax.sharding import PartitionSpec as P


NORM_EPS = 1e-5
PAD_COLS = 128
BLK = 512
BACK_BLK = 1024
VMEM = 67_043_328
F32 = jnp.float32
BF16 = jnp.bfloat16


ANY = pl.BlockSpec(memory_space=pl.ANY)


def whole(shape):
    return pl.BlockSpec(shape, lambda *_: (0,) * len(shape))


def params(n_axes):
    return pltpu.CompilerParams(
        dimension_semantics=("arbitrary",) * n_axes, vmem_limit_bytes=VMEM)


LOWEST = -3.4028234663852886e38


def fwd_body(k, n_parts, blk, limit_ref, wt_ref, *refs):
    a_refs = refs[:n_parts]
    z_ref, stat_ref, hold_ref = refs[-3:]
    step, steps = pl.program_id(0), pl.num_programs(0)
    pairs = [a_refs[i:i + 2] for i in range(0, n_parts, 2)]
    wide = 2 * a_refs[0].shape[0]

    def dots():
        for i, (lo, hi) in enumerate(pairs):
            a = jnp.concatenate([lo[...], hi[...]], axis=0)
            hold_ref[:, i * wide:(i + 1) * wide] = lax.dot_general(
                wt_ref[...], a, (((1,), (1,)), ((), ())), preferred_element_type=F32)

    def finish(masked):
        for i in range(len(pairs)):
            cols = slice(i * wide, (i + 1) * wide)
            z = hold_ref[:, cols]
            if masked:
                col = (step - 1) * blk + lax.broadcasted_iota(jnp.int32, z.shape, 0)
                z = jnp.where(col < limit_ref[0], z, -jnp.inf)
            z_ref[:, cols] = z
            old = stat_ref[k:k + 1, cols]
            new = jnp.maximum(old, jnp.max(z, axis=0, keepdims=True))
            total = jnp.sum(jnp.exp(z - new), axis=0, keepdims=True)
            stat_ref[k:k + 1, cols] = new
            stat_ref[4 + k:5 + k, cols] = stat_ref[4 + k:5 + k, cols] * jnp.exp(old - new) + total

    @pl.when(step == 0)
    def _():
        stat_ref[...] = jnp.zeros(stat_ref.shape, F32) if k == 0 else refs[n_parts][...]
        stat_ref[k:k + 1, :] = jnp.full((1, stat_ref.shape[1]), LOWEST, F32)
        stat_ref[4 + k:5 + k, :] = jnp.zeros((1, stat_ref.shape[1]), F32)
        dots()

    @pl.when((step > 0) & (step < steps - 1))
    def _():
        finish(False)
        dots()

    pl.when(step == steps - 1)(lambda: finish(True))


def fwd_call(k, parts, wt, limit, stats):
    vocab, dim = wt.shape
    toks = sum(p.shape[0] for p in parts)
    blocks = pl.cdiv(vocab, BLK)
    assert vocab - (blocks - 1) * BLK > PAD_COLS
    return pl.pallas_call(
        functools.partial(fwd_body, k, len(parts), BLK),
        grid=(blocks + 1,),
        in_specs=[pl.BlockSpec(memory_space=pltpu.SMEM), pl.BlockSpec((BLK, dim), lambda j: (jnp.minimum(j, blocks - 1), 0))]
        + [whole(p.shape) for p in parts] + [whole((8, toks))] * len(stats),
        out_specs=[pl.BlockSpec((BLK, toks), lambda j: (jnp.maximum(j - 1, 0), 0)), whole((8, toks))],
        out_shape=[jax.ShapeDtypeStruct((vocab, toks), F32), jax.ShapeDtypeStruct((8, toks), F32)],
        scratch_shapes=[pltpu.VMEM((BLK, toks), F32)],
        compiler_params=params(1),
        cost_estimate=pl.CostEstimate(
            flops=2 * vocab * dim * toks, bytes_accessed=vocab * dim * 2 + vocab * toks * 4,
            transcendentals=vocab * toks),
        name="fwd",
    )(limit, wt, *parts, *stats)


TILE = 1024


def mix(first, keep_ref, got_ref, outs):
    q = keep_ref[...] + got_ref[...]
    dhalf = q.shape[1] // 2

    @pl.when(first)
    def _():
        outs[0][...], outs[1][...] = q[:, :dhalf], q[:, dhalf:]

    @pl.when(jnp.logical_not(first))
    def _():
        outs[2][...], outs[3][...] = q[:, :dhalf], q[:, dhalf:]


def back_body(k, mixing, blk, vocab, label_ref, lse_ref, scale_ref, loss_ref, z_ref, wt_ref, *refs):
    dz_ref, keep_ref, send_ref, lost_ref = refs[-12:-8] if mixing else refs[-8:-4]
    acc_ref, w_ref, sem, w_sem = refs[-4:]
    step, steps = pl.program_id(0), pl.num_programs(0)
    tail = vocab - (vocab // blk) * blk or blk
    rows, dim = keep_ref.shape
    row = slice(k, k + 1)
    wide = dim // 2

    def fetch(block, size):
        slot = lax.rem(block, 2)
        at = pl.ds(pl.multiple_of(block * blk, blk), size)
        return [
            pltpu.make_async_copy(
                wt_ref.at[at, h * wide:(h + 1) * wide], w_ref.at[slot, 0:size, h * wide:(h + 1) * wide], w_sem.at[slot, h])
            for h in range(2)
        ]

    def begin(block, size):
        for c in fetch(block, size):
            c.start()

    pl.when(step == 0)(lambda: begin(step, blk))
    pl.when(step + 1 < steps - 1)(lambda: begin(step + 1, blk))
    pl.when(step + 1 == steps - 1)(lambda: begin(step + 1, tail))

    @pl.when(step == 0)
    def _():
        acc_ref[...] = jnp.zeros_like(acc_ref)
        lost_ref[...] = loss_ref[...]

    if mixing:
        mix(step < steps // 2, refs[0], refs[1], refs[-8:-4])

    def run(size, leave):
        arriving = fetch(step, size)
        arriving[0].wait()
        z = z_ref[:size]
        col = step * blk + lax.broadcasted_iota(jnp.int32, z.shape, 0)
        hit = col == label_ref[row]
        scale = scale_ref[row]
        dz = ((jnp.exp(z - lse_ref[row]) - jnp.where(hit, 1.0, 0.0)) * scale).astype(BF16)
        dz_ref[:size] = dz
        lost = jnp.sum(jnp.where(hit, z, 0.0), axis=0, keepdims=True) * scale
        part = lost_ref.shape[1]
        lost_ref[0:1] = lost_ref[0:1] - sum(lost[:, i:i + part] for i in range(0, lost.shape[1], part))
        copies, slot = [], lax.rem(step, 2)
        for t in range(dim // TILE):
            cols = slice(t * TILE, (t + 1) * TILE)
            if t * TILE == wide:
                arriving[1].wait()
            acc_ref[:, cols] += lax.dot_general(
                dz, w_ref[slot, :size, cols], (((0,), (0,)), ((), ())), preferred_element_type=F32)
            if leave:
                for h, out in enumerate((keep_ref, send_ref)):
                    copies.append(pltpu.make_async_copy(
                        acc_ref.at[h * rows:(h + 1) * rows, cols], out.at[:, cols], sem.at[2 * t + h]))
                    copies[-1].start()
        for c in copies:
            c.wait()

    pl.when(step < steps - 1)(lambda: run(blk, False))
    pl.when(step == steps - 1)(lambda: run(tail, True))


def back_call(k, z, wt, label, lse, scale, loss, shared, pair):
    vocab, dim = wt.shape
    toks = z.shape[1]
    rows = toks // 2
    steps = pl.cdiv(vocab, BACK_BLK)
    mixing = bool(pair)
    in_specs = [whole((8, toks))] * 3 + [whole((8, 128)), pl.BlockSpec((BACK_BLK, toks), lambda j: (j, 0)),
                                         ANY]
    out_specs = [pl.BlockSpec((BACK_BLK, toks), lambda j: (j, k)), ANY, ANY, whole((8, 128))]
    out_shape = [jax.ShapeDtypeStruct((vocab, 4 * toks), BF16), jax.ShapeDtypeStruct((rows, dim), F32),
                 jax.ShapeDtypeStruct((rows, dim), F32), jax.ShapeDtypeStruct((8, 128), F32)]
    if mixing:
        blk, mid, dhalf = rows // steps, steps // 2, dim // 2
        low = pl.BlockSpec((blk, dhalf), lambda j: (jnp.minimum(j, mid - 1), 0))
        high = pl.BlockSpec((blk, dhalf), lambda j: (jnp.maximum(j - mid, 0), 0))
        in_specs += [pl.BlockSpec((blk, dim), lambda j: (j, 0))] * 2
        out_specs += [low, low, high, high]
        out_shape += [jax.ShapeDtypeStruct((rows // 2, dhalf), F32)] * 4
    args = [label, lse, scale, loss, z, wt, *pair, *shared]
    return pl.pallas_call(
        functools.partial(back_body, k, mixing, BACK_BLK, vocab),
        grid=(steps,),
        in_specs=in_specs + [ANY] * len(shared),
        out_specs=out_specs,
        out_shape=out_shape,
        input_output_aliases={len(args) - 1: 0} if shared else {},
        scratch_shapes=[pltpu.VMEM((toks, dim), F32), pltpu.VMEM((2, BACK_BLK, dim), BF16),
                        pltpu.SemaphoreType.DMA((2 * dim // TILE,)), pltpu.SemaphoreType.DMA((2, 2))],
        compiler_params=params(1),
        cost_estimate=pl.CostEstimate(
            flops=2 * vocab * dim * toks, bytes_accessed=vocab * dim * 2 + vocab * toks * 6,
            transcendentals=vocab * toks),
        name="back",
    )(*args)


def weight_body(n_parts, dz_ref, keep_ref, got_ref, *refs):
    a_refs, out_ref, q_ref = refs[:n_parts], refs[-2], refs[-1]
    q_ref[...] = keep_ref[...] + got_ref[...]

    @pl.loop(0, out_ref.shape[1] // TILE)
    def _(k):
        cols = pl.ds(pl.multiple_of(k * TILE, TILE), TILE)
        a = jnp.concatenate([r[:, cols] for r in a_refs], axis=0)
        out_ref[:, cols] = jnp.dot(dz_ref[...], a, preferred_element_type=F32)


def weight_call(dz, parts, keep, got):
    vocab, toks = dz.shape
    dim = parts[0].shape[1]
    rows, cols = 1024, dim // 2
    blocks = pl.cdiv(vocab, rows)
    share = pl.BlockSpec((keep.shape[0] // (blocks * (dim // cols)), dim), lambda n, j: (n * blocks + j, 0))
    return pl.pallas_call(
        functools.partial(weight_body, len(parts)),
        grid=(dim // cols, blocks),
        in_specs=[pl.BlockSpec((rows, toks), lambda n, j: (j, 0)), share, share]
        + [pl.BlockSpec((p.shape[0], cols), lambda n, j: (0, n)) for p in parts],
        out_specs=[pl.BlockSpec((rows, cols), lambda n, j: (j, n)), share],
        out_shape=[jax.ShapeDtypeStruct((vocab, dim), F32), jax.ShapeDtypeStruct(keep.shape, F32)],
        compiler_params=params(2),
        cost_estimate=pl.CostEstimate(
            flops=2 * vocab * dim * toks, bytes_accessed=vocab * dim * 4 + vocab * toks * 4, transcendentals=0),
        name="dweight",
    )(dz, keep, got, *parts)


def norm_body(hid_ref, gain_ref, lo_ref, hi_ref):
    step = pl.program_id(0)
    x = hid_ref[...].astype(F32)
    inv = lax.rsqrt(jnp.mean(x * x, axis=-1, keepdims=True) + NORM_EPS)
    a = (x * inv * gain_ref[...]).astype(BF16)

    @pl.when(step < pl.num_programs(0) // 2)
    def _():
        lo_ref[...] = a

    @pl.when(step >= pl.num_programs(0) // 2)
    def _():
        hi_ref[...] = a


def norm_call(hidden, gain, order):
    rows, dim = hidden.shape
    steps = 2
    blk, mid = rows // steps, steps // 2
    body = lambda *refs: norm_body(refs[0], refs[1], refs[-2], refs[-1])
    return pl.pallas_call(
        body,
        grid=(steps,),
        in_specs=[pl.BlockSpec((blk, dim), lambda i: (i, 0)), whole((1, dim))] + [ANY] * len(order),
        out_specs=[pl.BlockSpec((blk, dim), lambda i: (jnp.minimum(i, mid - 1), 0)),
                   pl.BlockSpec((blk, dim), lambda i: (jnp.maximum(i - mid, 0), 0))],
        out_shape=[jax.ShapeDtypeStruct((rows // 2, dim), BF16)] * 2,
        compiler_params=params(1),
        cost_estimate=pl.CostEstimate(flops=5 * rows * dim, bytes_accessed=rows * dim * 4, transcendentals=rows),
        name="norm",
    )(hidden, gain[None], *order)


def peer(me, mask):
    out = me
    for bit in (1, 2, 4):
        if mask & bit:
            out = out + bit * (1 - 2 * ((me // bit) % 2))
    return out


def push_all(n, sends, send_sem, recv_sem):
    me = lax.axis_index("vp")
    barrier = pltpu.get_barrier_semaphore()
    for m in range(1, n):
        pl.semaphore_signal(barrier, inc=1, device_id={"vp": peer(me, m)}, device_id_type=pl.DeviceIdType.MESH)
    pl.semaphore_wait(barrier, n - 1)
    copies = [
        pltpu.make_async_remote_copy(
            src_ref=src, dst_ref=got.at[m], send_sem=send_sem.at[i, m], recv_sem=recv_sem.at[i, m],
            device_id={"vp": peer(me, m)}, device_id_type=pl.DeviceIdType.MESH)
        for m in range(1, n) for i, (src, got) in enumerate(sends)
    ]
    for c in copies:
        c.start()
    for c in copies:
        c.wait()


def tree(v):
    while len(v) > 1:
        v = [v[i] + v[i + 1] for i in range(0, len(v), 2)]
    return v[0]


def sum_body(n, gain_ref, loss_ref, gain_out, loss_out, got_gain, got_loss, send_sem, recv_sem):
    push_all(n, [(gain_ref, got_gain), (loss_ref, got_loss)], send_sem, recv_sem)
    gain = tree([gain_ref[...]] + [got_gain[m] for m in range(1, n)])
    per = gain.shape[1] // 128
    for i in range(gain.shape[0]):
        for j in range(per):
            gain_out[i * per + j:i * per + j + 1] = gain[i:i + 1, j * 128:(j + 1) * 128]
    loss = tree([loss_ref[...]] + [got_loss[m] for m in range(1, n)])
    loss_out[...] = jnp.sum(loss[0:1], axis=1, keepdims=True)


LAYOUT = (
    ((0, 0), (0, 1), (1, 0), (1, 1)),
    ((2, 0), (4, 0), (3, 0), (5, 0)),
    ((2, 1), (4, 1), (3, 1), (5, 1)),
    ((6, 0), (6, 1), (7, 0), (7, 1)),
)


def stats_body(n, vocab, stat_ref, label_ref, weight_ref, label_out, lse_out, scale_out, loss_out,
               got_stat, got_label, got_weight, send_sem, recv_sem):
    push_all(n, [(stat_ref, got_stat), (label_ref, got_label), (weight_ref, got_weight)], send_sem, recv_sem)
    width = stat_ref.shape[1] // 4
    base = lax.axis_index("vp") * vocab
    place = {key: (k, i) for k, row in enumerate(LAYOUT) for i, key in enumerate(row)}
    pick = lambda own, got, m, *at: own[at] if m == 0 else got[(m,) + at]
    lanes = lambda i: slice(i * width, (i + 1) * width)
    one = lambda k: slice(k, k + 1)
    total_weight = tree([
        jnp.sum(pick(weight_ref, got_weight, m, slice(0, 2)), axis=(0, 1), keepdims=True) for m in range(n)])
    loss = jnp.zeros((1, width), F32)
    label_out[4:] = jnp.zeros((4, 4 * width), jnp.int32)
    lse_out[4:] = jnp.zeros((4, 4 * width), F32)
    scale_out[4:] = jnp.zeros((4, 4 * width), F32)
    for k, row in enumerate(LAYOUT):
        for i, (r, h) in enumerate(row):
            tops, sums = [], []
            for m in range(n):
                kk, ii = place[(r ^ m, h)]
                tops.append(pick(stat_ref, got_stat, m, one(kk), lanes(ii)))
                sums.append(pick(stat_ref, got_stat, m, one(4 + kk), lanes(ii)))
            top = functools.reduce(jnp.maximum, tops)
            lse = top + jnp.log(tree([s * jnp.exp(t - top) for s, t in zip(sums, tops)]))
            scale = pick(weight_ref, got_weight, r, one(h)) / total_weight
            lse_out[one(k), lanes(i)] = lse
            scale_out[one(k), lanes(i)] = scale
            label_out[one(k), lanes(i)] = pick(label_ref, got_label, r, one(h)) - base
            if r == 0:
                loss = loss + scale * lse
    loss_out[...] = jnp.zeros(loss_out.shape, F32)
    loss_out[0:1] = loss


def small_call(body, n, args, outs, ident):
    vm = pl.BlockSpec(memory_space=pltpu.VMEM)
    sems = [pltpu.SemaphoreType.DMA((len(args), n))] * 2
    return pl.pallas_call(
        body,
        in_specs=[vm] * len(args),
        out_specs=[vm] * len(outs),
        out_shape=outs,
        scratch_shapes=[pltpu.VMEM((n,) + v.shape, v.dtype) for v in args] + sems,
        compiler_params=pltpu.CompilerParams(collective_id=ident, has_side_effects=True),
        cost_estimate=pl.CostEstimate(flops=4000, bytes_accessed=4_000_000, transcendentals=0),
    )(*args)


def mix_body(keep_ref, got_ref, a_ref, b_ref):
    q = keep_ref[...] + got_ref[...]
    dhalf = q.shape[1] // 2
    a_ref[...], b_ref[...] = q[:, :dhalf], q[:, dhalf:]


def mix_call(keep, got):
    rows, dim = keep.shape
    steps = 4
    blk, dhalf = rows // steps, dim // 2
    full = pl.BlockSpec((blk, dim), lambda i: (i, 0))
    return pl.pallas_call(
        mix_body,
        grid=(steps,),
        in_specs=[full, full],
        out_specs=[pl.BlockSpec((blk, dhalf), lambda i: (i, 0))] * 2,
        out_shape=[jax.ShapeDtypeStruct((rows, dhalf), F32)] * 2,
        compiler_params=params(1),
        cost_estimate=pl.CostEstimate(flops=rows * dim, bytes_accessed=rows * dim * 12, transcendentals=0),
        name="mix",
    )(keep, got)


def second_body(keep2_ref, keep4_ref, got2_ref, got4_ref, sa_ref, ta_ref, xa_ref, xb_ref, ya_ref, yb_ref,
                x2_ref, y4_ref, s_ref, t_ref):
    dhalf = sa_ref.shape[1]
    q2 = keep2_ref[...] + got2_ref[...]
    q4 = keep4_ref[...] + got4_ref[...]
    x2_ref[...] = q2[:, :dhalf]
    y4_ref[...] = q4[:, dhalf:]
    s_ref[0] = sa_ref[...] + xa_ref[...]
    s_ref[1] = q4[:, :dhalf] + xb_ref[...]
    t_ref[0] = ta_ref[...] + ya_ref[...]
    t_ref[1] = q2[:, dhalf:] + yb_ref[...]


def second_call(keep, got, sa, ta, x, y):
    half, dhalf = sa.shape
    steps = 4
    blk = half // steps
    at = lambda width, off: pl.BlockSpec((blk, width), lambda i: (i + off, 0))
    two = pl.BlockSpec((2, blk, dhalf), lambda i: (0, i, 0))
    return pl.pallas_call(
        second_body,
        grid=(steps,),
        in_specs=[at(2 * dhalf, 0), at(2 * dhalf, steps), at(2 * dhalf, 0), at(2 * dhalf, steps), at(dhalf, 0), at(dhalf, 0),
                  at(dhalf, 0), at(dhalf, steps), at(dhalf, 0), at(dhalf, steps)],
        out_specs=[at(dhalf, 0), at(dhalf, 0), two, two],
        out_shape=[jax.ShapeDtypeStruct((half, dhalf), F32)] * 2 + [jax.ShapeDtypeStruct((2, half, dhalf), F32)] * 2,
        compiler_params=params(1),
        cost_estimate=pl.CostEstimate(flops=8 * half * dhalf, bytes_accessed=half * dhalf * 80, transcendentals=0),
        name="second",
    )(keep, keep, got, got, sa, ta, x, x, y, y)


def last_body(hid_ref, gain_ref, q_ref, x2a_ref, x2b_ref, s4_ref, y4a_ref, y4b_ref, t2_ref, dh_ref, dgain_ref):
    step = pl.program_id(0)
    dhalf = s4_ref.shape[1]

    def run(x2_ref, y4_ref):
        q = q_ref[...]
        g = jnp.concatenate(
            [q[:, :dhalf] + x2_ref[...] + s4_ref[...], q[:, dhalf:] + y4_ref[...] + t2_ref[...]], axis=1)
        x = hid_ref[...].astype(F32)
        inv = lax.rsqrt(jnp.mean(x * x, axis=-1, keepdims=True) + NORM_EPS)
        norm = x * inv
        u = g * gain_ref[...]
        dh_ref[...] = (inv * (u - norm * jnp.mean(u * norm, axis=-1, keepdims=True))).astype(BF16)
        part = jnp.sum(g * norm, axis=0, keepdims=True)
        wide = dgain_ref.shape[1]
        for k in range(dgain_ref.shape[0]):
            piece = part[:, k * wide:(k + 1) * wide]
            dgain_ref[k:k + 1] = jnp.where(step == 0, piece, dgain_ref[k:k + 1] + piece)

    pl.when(step < pl.num_programs(0) // 2)(lambda: run(x2a_ref, y4a_ref))
    pl.when(step >= pl.num_programs(0) // 2)(lambda: run(x2b_ref, y4b_ref))


def last_call(hidden, gain, q, x2a, x2b, s4, y4a, y4b, t2):
    rows, dim = hidden.shape
    steps = 4
    blk, mid, dhalf = rows // steps, steps // 2, dim // 2
    row = lambda width: pl.BlockSpec((blk, width), lambda i: (i, 0))
    low = pl.BlockSpec((blk, dhalf), lambda i: (jnp.minimum(i, mid - 1), 0))
    high = pl.BlockSpec((blk, dhalf), lambda i: (jnp.maximum(i - mid, 0), 0))
    return pl.pallas_call(
        last_body,
        grid=(steps,),
        in_specs=[row(dim), whole((1, dim)), row(dim), low, high, row(dhalf), low, high, row(dhalf)],
        out_specs=[row(dim), whole((8, dim // 8))],
        out_shape=[jax.ShapeDtypeStruct((rows, dim), BF16), jax.ShapeDtypeStruct((8, dim // 8), F32)],
        compiler_params=params(1),
        cost_estimate=pl.CostEstimate(flops=20 * rows * dim, bytes_accessed=rows * dim * 20, transcendentals=rows),
        name="last",
    )(hidden, gain[None], q, x2a, x2b, s4, y4a, y4b, t2)


def solution(mesh):
    n = mesh.shape["vp"]

    def swap(v, mask):
        return lax.ppermute(v, "vp", [(i, i ^ mask) for i in range(n)])

    def compute(hidden, labels, loss_weight, norm_gain, w_local):
        rows, dim = hidden.shape
        half, dhalf = rows // 2, dim // 2
        wt = w_local.T
        vocab_local = wt.shape[0]
        vocab_real = vocab_local * n - PAD_COLS
        me = lax.axis_index("vp")

        limit = jnp.minimum(vocab_real - me * vocab_local, vocab_local).astype(jnp.int32).reshape(1)

        r0a, r0b = norm_call(hidden, norm_gain, [])
        r2a, r4a = swap(r0a, 2), swap(r0a, 4)
        r1a, r1b = swap(r0a, 1), swap(r0b, 1)
        r2b, r4b = swap(r0b, 2), swap(r0b, 4)
        r3a, r5a = swap(r2a, 1), swap(r4a, 1)
        r3b, r5b = swap(r2b, 1), swap(r4b, 1)
        r6a, r6b = swap(r2a, 4), swap(r4b, 2)
        r7a, r7b = swap(r6a, 1), swap(r6b, 1)
        groups = [[r0a, r0b, r1a, r1b], [r2a, r4a, r3a, r5a], [r2b, r4b, r3b, r5b], [r6a, r6b, r7a, r7b]]

        logits_g, stats = [], []
        for k, parts in enumerate(groups):
            logits, stat = fwd_call(k, parts, wt, limit, stats)
            logits_g.append(logits)
            stats = [stat]

        spec = jax.ShapeDtypeStruct
        label, lse, scale, loss = small_call(
            functools.partial(stats_body, n, vocab_local), n,
            [stats[0], labels.reshape(2, half), loss_weight.reshape(2, half)],
            [spec((8, 2 * rows), jnp.int32), spec((8, 2 * rows), F32), spec((8, 2 * rows), F32), spec((8, half), F32)],
            0)

        def back(k, loss, shared, pair):
            return back_call(k, logits_g[k], wt, label, lse, scale, loss, shared, pair)

        dz, keep3, send3, loss = back(3, loss, [], [])
        got3 = swap(send3, 1)
        dz, keep1, send1, loss = back(1, loss, [dz], [])
        q6x, q6y = mix_call(keep3, got3)
        x6, y6 = swap(q6x, 2), swap(q6y, 4)
        got1 = swap(send1, 1)
        dz, keep2, send2, loss = back(2, loss, [dz], [])
        got2 = swap(send2, 1)
        dz, keep0, send0, loss, x2a, ta, sa, y4a = back(0, loss, [dz], [keep1, got1])
        x2a, y4a = swap(x2a, 2), swap(y4a, 4)
        got0 = swap(send0, 1)
        x2b, y4b, s4, t2 = second_call(keep2, got2, sa, ta, x6, y6)
        x2b, y4b = swap(x2b, 2), swap(y4b, 4)
        s4, t2 = swap(s4, 4).reshape(rows, dhalf), swap(t2, 2).reshape(rows, dhalf)

        dwt, q0 = weight_call(dz, [p for g in groups for p in g], keep0, got0)
        d_input, d_gain = last_call(hidden, norm_gain, q0, x2a, x2b, s4, y4a, y4b, t2)
        d_gain, loss = small_call(
            functools.partial(sum_body, n), n, [d_gain, loss], [spec((dim // 128, 128), F32), spec((1, 1), F32)], 1)
        return loss.reshape(1), d_input, dwt.T, d_gain.reshape(dim)

    return jax.shard_map(
        compute,
        mesh=mesh,
        in_specs=(P(("dp", "vp"), None), P(("dp", "vp")), P(("dp", "vp")), P(None), P(None, "vp")),
        out_specs=(P("dp"), P(("dp", "vp"), None), P("dp", "vp"), P("dp")),
        check_vma=False,
    )
```
